8 devices in a mesh: dp: 2 (over y, z), tp: 4 (over x, core).
Axes of the slice: x: 2, y: 2, z: 1, core: 2. Of those that a mesh axis runs over, the one named last changes fastest.
Arguments:
- x: bfloat16 [256, 2048], P('dp'), parts along dimension 0
- w_gate: bfloat16 [2048, 6144], P(None, 'tp')
- w_up: bfloat16 [2048, 6144], P(None, 'tp')
- w_down: bfloat16 [6144, 2048], P('tp')
Outputs:
- output: bfloat16 [256, 2048], P('dp'), parts along dimension 0
There are 2 independent parts. The reference program is written for one: setup_inputs(seed, part) draws one part's arguments, and reference() takes and returns one part's arrays. A program takes and returns all parts, laid end to end along the dimension named above; an argument that names none is the same for every part.
All inputs are finite; a program needn't handle non-finite values.
Results may differ from the reference program's by a relative error of at most 0.016.
Values are sent between devices in bfloat16 or wider.
A program may use at most 2 GiB of HBM per device.

```python
import jax
import jax.numpy as jnp

ROWS = 128
D = 2048
FF = 6144


def setup_inputs(seed: int = 0, part: int = 0) -> dict:
    kx, kg, ku, kd = jax.random.split(jax.random.key(seed), 4)
    drawn = {
        "x": jax.random.normal(jax.random.fold_in(kx, part), (ROWS, D), jnp.float32),
        "w_gate": jax.random.normal(kg, (D, FF), jnp.float32) * D**-0.5,
        "w_up": jax.random.normal(ku, (D, FF), jnp.float32) * D**-0.5,
        "w_down": jax.random.normal(kd, (FF, D), jnp.float32) * FF**-0.5,
    }
    return {k: v.astype(jnp.bfloat16) for k, v in drawn.items()}


def reference(x, w_gate, w_up, w_down):
    gate = jnp.dot(x, w_gate, preferred_element_type=jnp.float32)
    up = jnp.dot(x, w_up, preferred_element_type=jnp.float32)
    hidden = (jax.nn.silu(gate) * up).astype(jnp.bfloat16)
    return jnp.dot(hidden, w_down, preferred_element_type=jnp.float32).astype(jnp.bfloat16)
```

```python
import jax
import jax.numpy as jnp
from jax import lax
from jax.experimental import pallas as pl
from jax.experimental.pallas import tpu as pltpu
from jax.sharding import PartitionSpec as P

ROWS = 128
D = 2048
F = 1536
FC = 256
NF = F // FC
HALF = D // 2
C = 256
NC = HALF // C


def kernel(
    x_hbm, wg_hbm, wu_hbm, wd_hbm, out,
    xv, wgv, wuv, wdv, h, tsend, trecv, own, ssend, srecv,
    x_sem, g_sem, u_sem, d_sem,
    ts_sem, tr_sem, ss_sem, sr_sem, ys_sem, yr_sem, yl_sem,
):
    me = lax.axis_index("tp")
    core = lax.rem(me, 2)
    sib = me + 1 - 2 * core
    opp = lax.rem(me + 2, 4)
    own_base = core * HALF
    sib_base = (1 - core) * HALF

    barrier = pltpu.get_barrier_semaphore()
    for other in (sib, opp):
        pl.semaphore_signal(barrier, inc=1, device_id={"tp": other}, device_id_type=pl.DeviceIdType.MESH)

    x_copy = pltpu.make_async_copy(x_hbm, xv, x_sem)
    x_copy.start()
    g_copies, u_copies, d_copies = [], [], []
    for j in range(NF):
        cols = pl.ds(j * FC, FC)
        g = pltpu.make_async_copy(wg_hbm.at[:, cols], wgv.at[j], g_sem.at[j])
        u = pltpu.make_async_copy(wu_hbm.at[:, cols], wuv.at[j], u_sem.at[j])
        g.start()
        u.start()
        g_copies.append(g)
        u_copies.append(u)
    for j in range(NC):
        for role, base in ((0, sib_base), (1, own_base)):
            cols = pl.ds(pl.multiple_of(base + j * C, C), C)
            d = pltpu.make_async_copy(wd_hbm.at[:, cols], wdv.at[2 * j + role], d_sem.at[2 * j + role])
            d.start()
            d_copies.append(d)

    x_copy.wait()
    for j in range(NF):
        g_copies[j].wait()
        gate = jnp.dot(xv[...], wgv[j], preferred_element_type=jnp.float32)
        u_copies[j].wait()
        up = jnp.dot(xv[...], wuv[j], preferred_element_type=jnp.float32)
        h[:, j * FC : (j + 1) * FC] = (jax.nn.silu(gate) * up).astype(jnp.bfloat16)

    pl.semaphore_wait(barrier, 2)

    def remote(src, dst, s, r, to):
        return pltpu.make_async_remote_copy(
            src_ref=src, dst_ref=dst, send_sem=s, recv_sem=r,
            device_id={"tp": to}, device_id_type=pl.DeviceIdType.MESH,
        )

    t_copies = [remote(tsend.at[j], trecv.at[j], ts_sem.at[j], tr_sem.at[j], sib) for j in range(NC)]
    s_copies = [remote(ssend.at[j], srecv.at[j], ss_sem.at[j], sr_sem.at[j], opp) for j in range(NC)]
    ysrc = ssend

    def down(j):
        d_copies[2 * j].wait()
        t = jnp.dot(h[...], wdv[2 * j], preferred_element_type=jnp.float32)
        tsend[j] = t.astype(jnp.bfloat16)
        t_copies[j].start()
        d_copies[2 * j + 1].wait()
        own[j] = jnp.dot(h[...], wdv[2 * j + 1], preferred_element_type=jnp.float32)

    def chip_sum(j):
        t_copies[j].wait_recv()
        ssend[j] = (own[j] + trecv[j].astype(jnp.float32)).astype(jnp.bfloat16)
        s_copies[j].start()

    for j in range(NC):
        down(j)
        if j >= 1:
            chip_sum(j - 1)
    chip_sum(NC - 1)

    y_copies = []
    for j in range(NC):
        s_copies[j].wait_recv()
        trecv[j] = (ssend[j].astype(jnp.float32) + srecv[j].astype(jnp.float32)).astype(jnp.bfloat16)
        cols = pl.ds(pl.multiple_of(own_base + j * C, C), C)
        yr = remote(trecv.at[j], out.at[:, cols], ys_sem.at[j], yr_sem.at[j], sib)
        yl = pltpu.make_async_copy(trecv.at[j], out.at[:, cols], yl_sem.at[j])
        yr.start()
        yl.start()
        y_copies.append((yr, yl))
    for j in range(NC):
        t_copies[j].wait_send()
        s_copies[j].wait_send()
        y_copies[j][1].wait()
        y_copies[j][0].wait()


def solution(mesh):
    bf, f32 = jnp.bfloat16, jnp.float32
    dma = pltpu.SemaphoreType.DMA

    def step(x, w_gate, w_up, w_down):
        hbm = lambda a: pltpu.with_memory_space_constraint(a, pltpu.HBM)
        return pl.pallas_call(
            kernel,
            out_shape=jax.ShapeDtypeStruct((ROWS, D), bf),
            in_specs=[pl.BlockSpec(memory_space=pl.ANY)] * 4,
            out_specs=pl.BlockSpec(memory_space=pl.ANY),
            scratch_shapes=[
                pltpu.VMEM((ROWS, D), bf),
                pltpu.VMEM((NF, D, FC), bf),
                pltpu.VMEM((NF, D, FC), bf),
                pltpu.VMEM((2 * NC, F, C), bf),
                pltpu.VMEM((ROWS, F), bf),
                pltpu.VMEM((NC, ROWS, C), bf),
                pltpu.VMEM((NC, ROWS, C), bf),
                pltpu.VMEM((NC, ROWS, C), f32),
                pltpu.VMEM((NC, ROWS, C), bf),
                pltpu.VMEM((NC, ROWS, C), bf),
                dma,
                dma((NF,)),
                dma((NF,)),
                dma((2 * NC,)),
                *[dma((NC,))] * 7,
            ],
            compiler_params=pltpu.CompilerParams(
                collective_id=0, has_side_effects=True, vmem_limit_bytes=60 * 2**20
            ),
        )(hbm(x), hbm(w_gate), hbm(w_up), hbm(w_down))

    return jax.shard_map(
        step,
        mesh=mesh,
        in_specs=(P("dp", None), P(None, "tp"), P(None, "tp"), P("tp", None)),
        out_specs=P("dp", None),
        check_vma=False,
    )
```

```python
import jax
import jax.numpy as jnp
from jax import lax
from jax.experimental import pallas as pl
from jax.experimental.pallas import tpu as pltpu
from jax.sharding import PartitionSpec as P

ROWS = 128
D = 2048
F = 1536
HALF = D // 2
HIDDEN = (256, 256, 256, 256, 256, 256)
C = 128
NC = HALF // C
LAG = 3
MESH = pl.DeviceIdType.MESH
scope = jax.named_scope


def remote(src, dst, send, recv, to):
    return pltpu.make_async_remote_copy(
        src_ref=src, dst_ref=dst, send_sem=send, recv_sem=recv, device_id={"tp": to}, device_id_type=MESH
    )


def block(x_hbm, wg_hbm, wu_hbm, wd_hbm, out, xv, wgv, wuv, wdv, h, tsend, trecv, own, ssend, srecv,
          in_sem, ts_sem, tr_sem, ss_sem, sr_sem, ys_sem, yr_sem):
    me = lax.axis_index("tp")
    core = lax.rem(me, 2)
    sib = me + 1 - 2 * core
    opp = lax.rem(me + 2, 4)

    barrier = pltpu.get_barrier_semaphore()
    for other in (sib, opp):
        pl.semaphore_signal(barrier, inc=1, device_id={"tp": other}, device_id_type=MESH)

    copies = []

    def load(src, dst):
        copies.append(pltpu.make_async_copy(src, dst, in_sem.at[len(copies)]))
        copies[-1].start()
        return copies[-1]

    x_copy = load(x_hbm, xv)
    hidden, at = [], 0
    for width in HIDDEN:
        cols = slice(at, at + width)
        at += width
        src = pl.ds(cols.start, width)
        hidden.append((cols, load(wg_hbm.at[:, src], wgv.at[:, src]), load(wu_hbm.at[:, src], wuv.at[:, src])))
    down = []
    for j in range(NC):
        for role in range(2):
            base = (1 - core if role == 0 else core) * HALF
            src = pl.ds(pl.multiple_of(base + j * C, C), C)
            down.append(load(wd_hbm.at[:, src], wdv.at[2 * j + role]))

    with scope("wait_x"):
        x_copy.wait()
    for k, (cols, g_copy, u_copy) in enumerate(hidden):
        with scope(f"wait_g{k}"):
            g_copy.wait()
            u_copy.wait()
        with scope(f"hid{k}"):
            gate = jnp.dot(xv[...], wgv[:, cols], preferred_element_type=jnp.float32)
            up = jnp.dot(xv[...], wuv[:, cols], preferred_element_type=jnp.float32)
            h[:, cols] = (jax.nn.silu(gate) * up).astype(jnp.bfloat16)
    with scope("barrier"):
        pl.semaphore_wait(barrier, 2)

    t_copies = [remote(tsend.at[j], trecv.at[j], ts_sem.at[j], tr_sem.at[j], sib) for j in range(NC)]
    s_copies = [remote(ssend.at[j], srecv.at[j], ss_sem.at[j], sr_sem.at[j], opp) for j in range(NC)]

    def chip_sum(j):
        with scope(f"wait_t{j}"):
            t_copies[j].wait_recv()
        with scope(f"sum{j}"):
            ssend[j] = (own[j] + trecv[j].astype(jnp.float32)).astype(jnp.bfloat16)
            s_copies[j].start()

    for j in range(NC):
        with scope(f"wait_d{j}"):
            down[2 * j].wait()
            down[2 * j + 1].wait()
        with scope(f"down{j}"):
            tsend[j] = jnp.dot(h[...], wdv[2 * j], preferred_element_type=jnp.float32).astype(jnp.bfloat16)
            t_copies[j].start()
            own[j] = jnp.dot(h[...], wdv[2 * j + 1], preferred_element_type=jnp.float32)
        if j >= LAG:
            chip_sum(j - LAG)
    for j in range(NC - LAG, NC):
        chip_sum(j)

    y_copies = []
    for j in range(NC):
        with scope(f"wait_s{j}"):
            s_copies[j].wait_recv()
        with scope(f"fin{j}"):
            out[core, j] = (ssend[j].astype(jnp.float32) + srecv[j].astype(jnp.float32)).astype(jnp.bfloat16)
            y_copies.append(remote(out.at[core, j], out.at[core, j], ys_sem.at[j], yr_sem.at[j], sib))
            y_copies[-1].start()
    with scope("drain_s"):
        for j in range(NC):
            t_copies[j].wait_send()
            s_copies[j].wait_send()
    with scope("drain_y"):
        for j in range(NC):
            y_copies[j].wait()


def store(y_vmem, y_hbm, sem):
    copies = []
    for c in range(2):
        for j in range(NC):
            dst = y_hbm.at[:, pl.ds(c * HALF + j * C, C)]
            copies.append(pltpu.make_async_copy(y_vmem.at[c, j], dst, sem.at[c * NC + j]))
            copies[-1].start()
    for copy in copies:
        copy.wait()


def solution(mesh):
    bf, f32 = jnp.bfloat16, jnp.float32
    dma = pltpu.SemaphoreType.DMA
    anywhere = pl.BlockSpec(memory_space=pl.ANY)
    vmem = pl.BlockSpec(memory_space=pltpu.VMEM)

    def step(x, w_gate, w_up, w_down):
        hbm = lambda a: pltpu.with_memory_space_constraint(a, pltpu.HBM)
        chunks = lambda dtype: pltpu.VMEM((NC, ROWS, C), dtype)
        y = pl.pallas_call(
            block,
            out_shape=pltpu.VMEM((2, NC, ROWS, C), bf),
            in_specs=[anywhere] * 4,
            out_specs=vmem,
            scratch_shapes=[
                pltpu.VMEM((ROWS, D), bf),
                pltpu.VMEM((D, F), bf),
                pltpu.VMEM((D, F), bf),
                pltpu.VMEM((2 * NC, F, C), bf),
                pltpu.VMEM((ROWS, F), bf),
                chunks(bf),
                chunks(bf),
                chunks(f32),
                chunks(bf),
                chunks(bf),
                dma((1 + 2 * len(HIDDEN) + 2 * NC,)),
                *[dma((NC,))] * 6,
            ],
            compiler_params=pltpu.CompilerParams(
                collective_id=0, has_side_effects=True, vmem_limit_bytes=50 * 2**20
            ),
            name="block",
        )(hbm(x), hbm(w_gate), hbm(w_up), hbm(w_down))
        return pl.pallas_call(
            store,
            out_shape=jax.ShapeDtypeStruct((ROWS, D), bf),
            in_specs=[vmem],
            out_specs=anywhere,
            scratch_shapes=[dma((2 * NC,))],
            name="store",
        )(pltpu.with_memory_space_constraint(y, pltpu.VMEM))

    return jax.shard_map(
        step,
        mesh=mesh,
        in_specs=(P("dp", None), P(None, "tp"), P(None, "tp"), P("tp", None)),
        out_specs=P("dp", None),
        check_vma=False,
    )
```

```python
import jax
import jax.numpy as jnp
from jax import lax
from jax.experimental import pallas as pl
from jax.experimental.pallas import tpu as pltpu
from jax.sharding import PartitionSpec as P

ROWS = 128
D = 2048
F = 1536
HIDDEN = (512, 512, 256, 256)
DOWN = (256, 256, 512, 1024)
C = 128
N = D // C
B = 2 * C
LAG = (1, 3)

OWNER = (0, 1, 0, 1, 0, 1, 0, 1, 0, 1, 0, 1, 1, 1, 1, 1)
DIRECT = (1,)
SHARED = (15,)
MESH = pl.DeviceIdType.MESH
scope = jax.named_scope


def columns(k):
    return pl.ds(k * C, C)


def block(x_hbm, wg_hbm, wu_hbm, wd_hbm, out, xv, wgv, wuv, wdv, h, own, tsend, trecv, ssend, srecv, drecv,
          in_sem, t_sem, s_sem, d_sem, y_sem, b_sem, send_sem):
    me = lax.axis_index("tp")
    core = lax.rem(me, 2)
    sib = me + 1 - 2 * core
    opp = lax.rem(me + 2, 4)
    cross = 3 - me
    f32 = jnp.float32

    barrier = pltpu.get_barrier_semaphore()
    for other in (sib, opp, cross):
        pl.semaphore_signal(barrier, inc=1, device_id={"tp": other}, device_id_type=MESH)

    copies = []

    def load(src, dst):
        copies.append(pltpu.make_async_copy(src, dst, in_sem.at[len(copies)]))
        copies[-1].start()
        return copies[-1]

    x_copy = load(x_hbm, xv)
    hidden, at = [], 0
    for width in HIDDEN:
        src = pl.ds(at, width)
        hidden.append((slice(at, at + width), load(wg_hbm.at[:, src], wgv.at[:, src]), load(wu_hbm.at[:, src], wuv.at[:, src])))
        at += width
    down, at = {}, 0
    for width in DOWN:
        src = pl.ds(at, width)
        down[at] = load(wd_hbm.at[:, src], wdv.at[:, src])
        at += width

    with scope("wait_x"):
        x_copy.wait()
    for k, (cols, g_copy, u_copy) in enumerate(hidden):
        with scope(f"wait_g{k}"):
            g_copy.wait()
            u_copy.wait()
        with scope(f"hid{k}"):
            gate = jnp.dot(xv[...], wgv[:, cols], preferred_element_type=f32)
            up = jnp.dot(xv[...], wuv[:, cols], preferred_element_type=f32)
            h[:, cols] = (jax.nn.silu(gate) * up).astype(jnp.bfloat16)
    with scope("barrier"):
        pl.semaphore_wait(barrier, 3)

    def remote(src, dst, recv, to):
        return pltpu.make_async_remote_copy(
            src_ref=src, dst_ref=dst, send_sem=send_sem, recv_sem=recv, device_id={"tp": to}, device_id_type=MESH
        )

    slot = [OWNER[:k].count(OWNER[k]) for k in range(N)]
    t_copy = lambda k: remote(tsend.at[k], trecv.at[k], t_sem.at[slot[k]], sib)
    s_copy = lambda k, to: remote(ssend.at[k], srecv.at[k], s_sem.at[slot[k]], to)
    b_copy = lambda k: remote(ssend.at[k], ssend.at[k], b_sem.at[SHARED.index(k)], sib)
    y_copy = lambda k: remote(out.at[:, columns(k)], out.at[:, columns(k)], y_sem, sib)
    direct = [k for k in range(N) if k in DIRECT]
    shared = [k for k in range(N) if k in SHARED]
    sent = {0: 0, 1: 0}

    def term(j):
        if j * B in down:
            with scope(f"wait_d{j}"):
                down[j * B].wait()
        with scope(f"down{j}"):
            value = jnp.dot(h[...], wdv[:, j * B : (j + 1) * B], preferred_element_type=f32)
            for i in range(B // C):
                k = j * (B // C) + i
                part = value[:, i * C : (i + 1) * C]
                own[k] = part
                tsend[k] = part.astype(jnp.bfloat16)
            for i in range(B // C):
                k = j * (B // C) + i
                if k in DIRECT:
                    i = direct.index(k)
                    for c in range(2):
                        to = opp if c == OWNER[k] else cross
                        sent[c] += 1

                        @pl.when(core == c)
                        def _(to=to, i=i, c=c, k=k):
                            remote(tsend.at[k], drecv.at[2 * i + c], d_sem.at[2 * i + c], to).start()

                sent[1 - OWNER[k]] += 1

                @pl.when(core != OWNER[k])
                def _(k=k):
                    t_copy(k).start()

    def chip_sum(j, c):
        chunks = [k for k in range(j * (B // C), (j + 1) * (B // C)) if OWNER[k] == c and k not in DIRECT]
        sent[c] += len(chunks) + 2 * len([k for k in chunks if k in SHARED])

        @pl.when(core == c)
        def _():
            for k in chunks:
                with scope(f"wait_t{k}"):
                    t_copy(k).wait_recv()
                with scope(f"sum{k}"):
                    ssend[k] = (own[k] + trecv[k].astype(f32)).astype(jnp.bfloat16)
                    if k in SHARED:
                        s_copy(k, cross).start()
                    s_copy(k, opp).start()
                    if k in SHARED:
                        b_copy(k).start()

    steps = D // B
    for j in range(steps + max(LAG)):
        if j < steps:
            term(j)
        for c in range(2):
            if 0 <= j - LAG[c] < steps:
                chip_sum(j - LAG[c], c)

    for c in range(2):
        mine = [k for k in range(N) if OWNER[k] == c and k not in SHARED]
        theirs = [k for k in range(N) if OWNER[k] != c and k not in SHARED]
        sent[c] += len(mine)

        @pl.when(core == c)
        def _(c=c, mine=mine, theirs=theirs):
            for k in mine:
                if k in DIRECT:
                    i = direct.index(k)
                    with scope(f"wait_s{k}"):
                        t_copy(k).wait_recv()
                        for p in range(2):
                            remote(tsend.at[k], drecv.at[2 * i + p], d_sem.at[2 * i + p], opp).wait_recv()
                    here = tsend[k].astype(f32) + trecv[k].astype(f32)
                    there = drecv[2 * i + c].astype(f32) + drecv[2 * i + 1 - c].astype(f32)
                else:
                    with scope(f"wait_s{k}"):
                        s_copy(k, opp).wait_recv()
                    here, there = ssend[k].astype(f32), srecv[k].astype(f32)
                with scope(f"fin{k}"):
                    out[:, columns(k)] = (here + there).astype(jnp.bfloat16)
                    y_copy(k).start()
            for k in shared:
                with scope(f"wait_s{k}"):
                    s_copy(k, opp).wait_recv()
                    if OWNER[k] != c:
                        b_copy(k).wait_recv()
                with scope(f"fin{k}"):
                    out[:, columns(k)] = (ssend[k].astype(f32) + srecv[k].astype(f32)).astype(jnp.bfloat16)
            with scope("drain_send"):
                every = tsend.at[pl.ds(0, N)]
                total = sent[c]
                while total:
                    n = min(total, N)
                    remote(tsend.at[pl.ds(0, n)], trecv.at[pl.ds(0, n)], y_sem, sib).wait_send()
                    total -= n
            with scope("drain_y"):
                n = len(theirs)
                remote(tsend.at[pl.ds(0, n)], trecv.at[pl.ds(0, n)], y_sem, sib).wait_recv()


def store(y_vmem, y_hbm, sem):
    copy = pltpu.make_async_copy(y_vmem, y_hbm, sem)
    copy.start()
    copy.wait()


def solution(mesh):
    bf = jnp.bfloat16
    dma = pltpu.SemaphoreType.DMA
    anywhere = pl.BlockSpec(memory_space=pl.ANY)
    vmem = pl.BlockSpec(memory_space=pltpu.VMEM)

    def step(x, w_gate, w_up, w_down):
        hbm = lambda a: pltpu.with_memory_space_constraint(a, pltpu.HBM)
        chunks = lambda n, dtype: pltpu.VMEM((n, ROWS, C), dtype)
        y = pl.pallas_call(
            block,
            out_shape=pltpu.VMEM((ROWS, D), bf),
            in_specs=[anywhere] * 4,
            out_specs=vmem,
            scratch_shapes=[
                pltpu.VMEM((ROWS, D), bf),
                pltpu.VMEM((D, F), bf),
                pltpu.VMEM((D, F), bf),
                pltpu.VMEM((F, D), bf),
                pltpu.VMEM((ROWS, F), bf),
                chunks(N, jnp.float32),
                chunks(N, bf),
                chunks(N, bf),
                chunks(N, bf),
                chunks(N, bf),
                chunks(2 * max(1, len(DIRECT)), bf),
                dma((1 + 2 * len(HIDDEN) + len(DOWN),)),
                dma((max(OWNER.count(0), OWNER.count(1)),)),
                dma((max(OWNER.count(0), OWNER.count(1)),)),
                dma((2 * max(1, len(DIRECT)),)),
                dma,
                dma((max(1, len(SHARED)),)),
                dma,
            ],
            compiler_params=pltpu.CompilerParams(
                collective_id=0, has_side_effects=True, vmem_limit_bytes=50 * 2**20
            ),
            name="block",
        )(hbm(x), hbm(w_gate), hbm(w_up), hbm(w_down))
        return pl.pallas_call(
            store,
            out_shape=jax.ShapeDtypeStruct((ROWS, D), bf),
            in_specs=[vmem],
            out_specs=anywhere,
            scratch_shapes=[dma],
            name="store",
        )(pltpu.with_memory_space_constraint(y, pltpu.VMEM))

    return jax.shard_map(
        step,
        mesh=mesh,
        in_specs=(P("dp", None), P(None, "tp"), P(None, "tp"), P("tp", None)),
        out_specs=P("dp", None),
        check_vma=False,
    )
```

```python
import jax
import jax.numpy as jnp
from jax import lax
from jax.experimental import pallas as pl
from jax.experimental.pallas import tpu as pltpu
from jax.sharding import PartitionSpec as P

ROWS = 128
D = 2048
F = 1536
HIDDEN = ((768, (1024, 1024)), (768, (1024, 512, 512)))
DOWN = (256, 256, 512, 1024)
C = 128
N = D // C
STEPS = ((0, 1), (2, 3), (4, 5, 6, 7), (8, 9, 10, 11), (12, 13, 14, 15))
LAG = (1, 2)

GROUPS = (((0, 2), (4, 6), (8,), (10,)), ((5, 7), (9, 11), (12, 13), (14,)))
DIRECT = (1, 3)
SHARED = (15,)
MESH = pl.DeviceIdType.MESH
scope = jax.named_scope
OWNER = {k: c for c in range(2) for group in GROUPS[c] for k in group} | {k: 1 for k in DIRECT + SHARED}


def columns(k):
    return pl.ds(k * C, C)


def block(x_hbm, wg_hbm, wu_hbm, wd_hbm, out, xv, guv, part, wdv, h, own, tsend, trecv, ssend, srecv, drecv,
          in_sem, t_sem, s_sem, d_sem, y_sem, b_sem, send_sem):
    me = lax.axis_index("tp")
    core = lax.rem(me, 2)
    sib = me + 1 - 2 * core
    opp = lax.rem(me + 2, 4)
    cross = 3 - me
    f32 = jnp.float32

    barrier = pltpu.get_barrier_semaphore()
    for other in (sib, opp, cross):
        pl.semaphore_signal(barrier, inc=1, device_id={"tp": other}, device_id_type=MESH)

    n_sem = 0

    def load(*pairs):
        nonlocal n_sem
        for src, dst in pairs:
            pltpu.make_async_copy(src, dst, in_sem.at[n_sem]).start()
        n_sem += 1
        return n_sem - 1

    def loaded(ref, n):
        pltpu.make_async_copy(ref, ref, in_sem.at[n]).wait()

    x_copy = load((x_hbm, xv))
    hidden, at = [], 0
    for width, depths in HIDDEN:
        cols, top, pieces = pl.ds(at, width), 0, []
        for depth in depths:
            rows = pl.ds(top, depth)
            n = load((wg_hbm.at[rows, cols], guv.at[0, rows, cols]), (wu_hbm.at[rows, cols], guv.at[1, rows, cols]))
            pieces.append((n, top, depth))
            top += depth
        hidden.append((at, width, pieces))
        at += width
    down, at = {}, 0
    for width in DOWN:
        cols = pl.ds(at, width)
        down[at // C] = (load((wd_hbm.at[:, cols], wdv.at[:, cols])), cols)
        at += width

    with scope("wait_x"):
        loaded(xv, x_copy)
    for c, (at, width, pieces) in enumerate(hidden):
        cols = slice(at, at + width)
        for n, top, depth in pieces:
            with scope(f"wait_g{c}_{top}"):
                loaded(guv.at[:, pl.ds(top, depth), pl.ds(at, width)], n)
            with scope(f"hid{c}_{top}"):
                rows = slice(top, top + depth)
                gate = jnp.dot(xv[:, rows], guv[0, rows, cols], preferred_element_type=f32)
                up = jnp.dot(xv[:, rows], guv[1, rows, cols], preferred_element_type=f32)
                if top > 0:
                    gate, up = gate + part[0, :, :width], up + part[1, :, :width]
                if top + depth < D:
                    part[0, :, :width], part[1, :, :width] = gate, up
                else:
                    h[:, cols] = (jax.nn.silu(gate) * up).astype(jnp.bfloat16)
    with scope("barrier"):
        pl.semaphore_wait(barrier, 3)

    def remote(src, dst, recv, to):
        return pltpu.make_async_remote_copy(
            src_ref=src, dst_ref=dst, send_sem=send_sem, recv_sem=recv, device_id={"tp": to}, device_id_type=MESH
        )

    def wait_recv(sem, n):
        remote(tsend.at[pl.ds(0, n)], trecv.at[pl.ds(0, n)], sem, sib).wait_recv()

    group_of = {k: g for c in range(2) for g, group in enumerate(GROUPS[c]) for k in group}
    shared_sem = s_sem.at[max(len(groups) for groups in GROUPS)]
    s_copy = lambda k, to: remote(ssend.at[k], srecv.at[k], shared_sem if k in SHARED else s_sem.at[group_of[k]], to)
    y_copy = lambda k: remote(out.at[:, columns(k)], out.at[:, columns(k)], y_sem, sib)
    sent = {0: 0, 1: 0}

    def term(j):
        chunks = STEPS[j]
        if chunks[0] in down:
            n, cols = down[chunks[0]]
            with scope(f"wait_d{j}"):
                loaded(wdv.at[:, cols], n)
        with scope(f"down{j}"):
            value = jnp.dot(h[...], wdv[:, chunks[0] * C : (chunks[-1] + 1) * C], preferred_element_type=f32)
            for i, k in enumerate(chunks):
                own[k] = value[:, i * C : (i + 1) * C]
                tsend[k] = value[:, i * C : (i + 1) * C].astype(jnp.bfloat16)
            for c in range(2):

                @pl.when(core == c)
                def _(c=c):
                    for k in chunks:
                        if k in DIRECT:
                            place = drecv.at[2 * DIRECT.index(k) + c]
                            remote(tsend.at[k], place, d_sem, opp if c == OWNER[k] else cross).start()
                            sent[c] += 1
                    for k in chunks:
                        if OWNER[k] != c:
                            remote(tsend.at[k], trecv.at[k], t_sem.at[j], sib).start()
                            sent[c] += 1

    def chip_sum(j, c):
        chunks = [k for k in STEPS[j] if OWNER[k] == c]

        @pl.when(core == c)
        def _():
            if any(k not in DIRECT for k in chunks):
                with scope(f"wait_t{j}"):
                    wait_recv(t_sem.at[j], len(chunks))
            for k in chunks:
                if k in DIRECT:
                    continue
                with scope(f"sum{k}"):
                    ssend[k] = (own[k] + trecv[k].astype(f32)).astype(jnp.bfloat16)
                    if k in SHARED:
                        s_copy(k, cross).start()
                    s_copy(k, opp).start()
                    if k in SHARED:
                        remote(ssend.at[k], ssend.at[k], b_sem, sib).start()
                    sent[c] += 3 if k in SHARED else 1

    for j in range(len(STEPS) + max(LAG)):
        if j < len(STEPS):
            term(j)
        for c in range(2):
            if 0 <= j - LAG[c] < len(STEPS):
                chip_sum(j - LAG[c], c)

    for c in range(2):

        @pl.when(core == c)
        def _(c=c):
            def finish(k, here, there):
                with scope(f"fin{k}"):
                    out[:, columns(k)] = (here + there).astype(jnp.bfloat16)
                    if k not in SHARED:
                        y_copy(k).start()
                        sent[c] += 1

            if c == 1 and DIRECT:
                with scope("wait_direct"):
                    wait_recv(d_sem, 2 * len(DIRECT))
                    for j, chunks in enumerate(STEPS):
                        mine = [k for k in chunks if OWNER[k] == 1]
                        if mine and all(k in DIRECT for k in mine):
                            wait_recv(t_sem.at[j], len(mine))
                for i, k in enumerate(DIRECT):
                    here = tsend[k].astype(f32) + trecv[k].astype(f32)
                    finish(k, here, drecv[2 * i + 1].astype(f32) + drecv[2 * i].astype(f32))
            for group in GROUPS[c]:
                with scope(f"wait_s{group[0]}"):
                    wait_recv(s_sem.at[group_of[group[0]]], len(group))
                for k in group:
                    finish(k, ssend[k].astype(f32), srecv[k].astype(f32))
            if SHARED:
                with scope("wait_shared"):
                    wait_recv(shared_sem, len(SHARED))
                    if c == 0:
                        wait_recv(b_sem, len(SHARED))
            for k in SHARED:
                finish(k, ssend[k].astype(f32), srecv[k].astype(f32))
            with scope("drain_send"):
                total = sent[c]
                while total:
                    n = min(total, N)
                    remote(tsend.at[pl.ds(0, n)], trecv.at[pl.ds(0, n)], y_sem, sib).wait_send()
                    total -= n
            with scope("drain_y"):
                wait_recv(y_sem, len([k for k in range(N) if OWNER[k] != c and k not in SHARED]))


def store(y_vmem, y_hbm, sem):
    copy = pltpu.make_async_copy(y_vmem, y_hbm, sem)
    copy.start()
    copy.wait()


def solution(mesh):
    bf = jnp.bfloat16
    dma = pltpu.SemaphoreType.DMA
    anywhere = pl.BlockSpec(memory_space=pl.ANY)
    vmem = pl.BlockSpec(memory_space=pltpu.VMEM)

    def step(x, w_gate, w_up, w_down):
        hbm = lambda a: pltpu.with_memory_space_constraint(a, pltpu.HBM)
        chunks = lambda n, dtype: pltpu.VMEM((n, ROWS, C), dtype)
        y = pl.pallas_call(
            block,
            out_shape=pltpu.VMEM((ROWS, D), bf),
            in_specs=[anywhere] * 4,
            out_specs=vmem,
            scratch_shapes=[
                pltpu.VMEM((ROWS, D), bf),
                pltpu.VMEM((2, D, F), bf),
                pltpu.VMEM((2, ROWS, max(width for width, _ in HIDDEN)), jnp.float32),
                pltpu.VMEM((F, D), bf),
                pltpu.VMEM((ROWS, F), bf),
                chunks(N, jnp.float32),
                chunks(N, bf),
                chunks(N, bf),
                chunks(N, bf),
                chunks(N, bf),
                chunks(2 * max(1, len(DIRECT)), bf),
                dma((1 + sum(len(depths) for _, depths in HIDDEN) + len(DOWN),)),
                dma((len(STEPS),)),
                dma((1 + max(len(groups) for groups in GROUPS),)),
                *[dma] * 4,
            ],
            compiler_params=pltpu.CompilerParams(
                collective_id=0, has_side_effects=True, vmem_limit_bytes=50 * 2**20
            ),
            name="block",
        )(hbm(x), hbm(w_gate), hbm(w_up), hbm(w_down))
        return pl.pallas_call(
            store,
            out_shape=jax.ShapeDtypeStruct((ROWS, D), bf),
            in_specs=[vmem],
            out_specs=anywhere,
            scratch_shapes=[dma],
            name="store",
        )(pltpu.with_memory_space_constraint(y, pltpu.VMEM))

    return jax.shard_map(
        step,
        mesh=mesh,
        in_specs=(P("dp", None), P(None, "tp"), P(None, "tp"), P("tp", None)),
        out_specs=P("dp", None),
        check_vma=False,
    )
```

```python
import jax
import jax.numpy as jnp
from jax import lax
from jax.experimental import pallas as pl
from jax.experimental.pallas import tpu as pltpu
from jax.sharding import PartitionSpec as P

ROWS = 128
D = 2048
F = 1536
HIDDEN = ((768, (1024, 1024)), (768, (1024, 512, 512)))
DOWN = (256, 256, 512, 1024)
C = 128
N = D // C
STEPS = ((0, 1), (2, 3), (4, 5, 6, 7), (8, 9, 10, 11), (12, 13, 14, 15))
SPLIT = (0, 1)
LAG = ((1, 1, 0, 1, 1), (2, 2, 2, 2, 2))

GROUPS = (((0, 2), (4, 6), (8,), (10,)), ((5, 7), (9, 11), (12,),(13,)))
DIRECT = (1, 3)
SHARED = (14,15)
MESH = pl.DeviceIdType.MESH
scope = jax.named_scope
OWNER = {k: c for c in range(2) for group in GROUPS[c] for k in group} | {k: 1 for k in DIRECT + SHARED}


def columns(k):
    return pl.ds(k * C, C)


def block(x_hbm, wg_hbm, wu_hbm, wd_hbm, out, xv, guv, part, wdv, h, own, tsend, trecv, ssend, srecv, drecv,
          in_sem, t_sem, s_sem, d_sem, y_sem, b_sem, send_sem):
    me = lax.axis_index("tp")
    core = lax.rem(me, 2)
    sib = me + 1 - 2 * core
    opp = lax.rem(me + 2, 4)
    cross = 3 - me
    f32 = jnp.float32

    barrier = pltpu.get_barrier_semaphore()
    for other in (sib, opp, cross):
        pl.semaphore_signal(barrier, inc=1, device_id={"tp": other}, device_id_type=MESH)

    n_sem = 0

    def load(*pairs):
        nonlocal n_sem
        for src, dst in pairs:
            pltpu.make_async_copy(src, dst, in_sem.at[n_sem]).start()
        n_sem += 1
        return n_sem - 1

    def loaded(ref, n):
        pltpu.make_async_copy(ref, ref, in_sem.at[n]).wait()

    x_copy = load((x_hbm, xv))
    hidden, at = [], 0
    for width, depths in HIDDEN:
        cols, top, pieces = pl.ds(at, width), 0, []
        for depth in depths:
            rows = pl.ds(top, depth)
            n = load((wg_hbm.at[rows, cols], guv.at[0, rows, cols]), (wu_hbm.at[rows, cols], guv.at[1, rows, cols]))
            pieces.append((n, top, depth))
            top += depth
        hidden.append((at, width, pieces))
        at += width
    down, at = {}, 0
    for width in DOWN:
        cols = pl.ds(at, width)
        down[at // C] = (load((wd_hbm.at[:, cols], wdv.at[:, cols])), cols)
        at += width

    with scope("wait_x"):
        loaded(xv, x_copy)
    for c, (at, width, pieces) in enumerate(hidden):
        cols = slice(at, at + width)
        for n, top, depth in pieces:
            with scope(f"wait_g{c}_{top}"):
                loaded(guv.at[:, pl.ds(top, depth), pl.ds(at, width)], n)
            with scope(f"hid{c}_{top}"):
                rows = slice(top, top + depth)
                gate = jnp.dot(xv[:, rows], guv[0, rows, cols], preferred_element_type=f32)
                up = jnp.dot(xv[:, rows], guv[1, rows, cols], preferred_element_type=f32)
                if top > 0:
                    gate, up = gate + part[0, :, :width], up + part[1, :, :width]
                if top + depth < D:
                    part[0, :, :width], part[1, :, :width] = gate, up
                else:
                    h[:, cols] = (jax.nn.silu(gate) * up).astype(jnp.bfloat16)
    def remote(src, dst, recv, to):
        return pltpu.make_async_remote_copy(
            src_ref=src, dst_ref=dst, send_sem=send_sem, recv_sem=recv, device_id={"tp": to}, device_id_type=MESH
        )

    def wait_recv(sem, n):
        remote(tsend.at[pl.ds(0, n)], trecv.at[pl.ds(0, n)], sem, sib).wait_recv()

    group_of = {k: g for c in range(2) for g, group in enumerate(GROUPS[c]) for k in group}
    shared_sem = s_sem.at[max(len(groups) for groups in GROUPS)]
    s_copy = lambda k, to: remote(ssend.at[k], srecv.at[k], shared_sem if k in SHARED else s_sem.at[group_of[k]], to)
    y_copy = lambda k: remote(out.at[:, columns(k)], out.at[:, columns(k)], y_sem, sib)
    sent = {0: 0, 1: 0}

    def term(j):
        chunks = STEPS[j]
        if chunks[0] in down:
            n, cols = down[chunks[0]]
            with scope(f"wait_d{j}"):
                loaded(wdv.at[:, cols], n)
        with scope(f"down{j}"):
            cols = slice(chunks[0] * C, (chunks[-1] + 1) * C)
            if j in SPLIT:
                width = len(chunks) * C
                half = [slice(0, F // 2), slice(F // 2, F)]
                part[me // 4, :, :width] = jnp.dot(h[:, half[0]], wdv[half[0], cols], preferred_element_type=f32)
                value = jnp.dot(h[:, half[1]], wdv[half[1], cols], preferred_element_type=f32) + part[0, :, :width]
            else:
                value = jnp.dot(h[...], wdv[:, cols], preferred_element_type=f32)
            for i, k in enumerate(chunks):
                own[k] = value[:, i * C : (i + 1) * C]
                tsend[k] = value[:, i * C : (i + 1) * C].astype(jnp.bfloat16)
            if j == 0:
                pl.semaphore_wait(barrier, 3)
            for c in range(2):

                @pl.when(core == c)
                def _(c=c):
                    for k in chunks:
                        if k in DIRECT:
                            place = drecv.at[2 * DIRECT.index(k) + c]
                            remote(tsend.at[k], place, d_sem, opp if c == OWNER[k] else cross).start()
                            sent[c] += 1
                    for k in chunks:
                        if OWNER[k] != c:
                            remote(tsend.at[k], trecv.at[k], t_sem.at[j], sib).start()
                            sent[c] += 1

    def chip_sum(j, c):
        mine = [k for k in STEPS[j] if OWNER[k] == c]
        chunks = [k for k in mine if k not in DIRECT]
        if not chunks:
            return
        sent[c] += len(chunks) + 2 * len([k for k in chunks if k in SHARED])

        @pl.when(core == c)
        def _():
            with scope(f"wait_t{j}"):
                wait_recv(t_sem.at[j], len(mine))
            for k in chunks:
                with scope(f"sum{k}"):
                    ssend[k] = (own[k] + trecv[k].astype(f32)).astype(jnp.bfloat16)
                    if k in SHARED:
                        s_copy(k, cross).start()
                        remote(ssend.at[k], ssend.at[k], b_sem, sib).start()
                    else:
                        s_copy(k, opp).start()
            for k in chunks:
                if k in SHARED:
                    s_copy(k, opp).start()

    for j in range(len(STEPS) + 3):
        if j < len(STEPS):
            term(j)
        for c in range(2):
            for k in range(len(STEPS)):
                if k + LAG[c][k] == j:
                    chip_sum(k, c)

    for c in range(2):

        @pl.when(core == c)
        def _(c=c):
            def finish(k, here, there):
                with scope(f"fin{k}"):
                    out[:, columns(k)] = (here + there).astype(jnp.bfloat16)
                    if k not in SHARED:
                        y_copy(k).start()
                        sent[c] += 1

            if c == 1 and DIRECT:
                with scope("wait_direct"):
                    wait_recv(d_sem, 2 * len(DIRECT))
                    for j, chunks in enumerate(STEPS):
                        mine = [k for k in chunks if OWNER[k] == 1]
                        if mine and all(k in DIRECT for k in mine):
                            wait_recv(t_sem.at[j], len(mine))
                for i, k in enumerate(DIRECT):
                    here = tsend[k].astype(f32) + trecv[k].astype(f32)
                    finish(k, here, drecv[2 * i + 1].astype(f32) + drecv[2 * i].astype(f32))
            for group in GROUPS[c]:
                with scope(f"wait_s{group[0]}"):
                    wait_recv(s_sem.at[group_of[group[0]]], len(group))
                for k in group:
                    finish(k, ssend[k].astype(f32), srecv[k].astype(f32))
            if SHARED:
                with scope("wait_shared"):
                    wait_recv(shared_sem, len(SHARED))
                    if c == 0:
                        wait_recv(b_sem, len(SHARED))
            for k in SHARED:
                finish(k, ssend[k].astype(f32), srecv[k].astype(f32))
            with scope("drain_send"):
                total = sent[c]
                while total:
                    n = min(total, N)
                    remote(tsend.at[pl.ds(0, n)], trecv.at[pl.ds(0, n)], y_sem, sib).wait_send()
                    total -= n
            with scope("drain_y"):
                wait_recv(y_sem, len([k for k in range(N) if OWNER[k] != c and k not in SHARED]))


def solution(mesh):
    bf = jnp.bfloat16
    dma = pltpu.SemaphoreType.DMA
    anywhere = pl.BlockSpec(memory_space=pl.ANY)
    vmem = pl.BlockSpec(memory_space=pltpu.VMEM)

    def step(x, w_gate, w_up, w_down):
        hbm = lambda a: pltpu.with_memory_space_constraint(a, pltpu.HBM)
        chunks = lambda n, dtype: pltpu.VMEM((n, ROWS, C), dtype)
        return pl.pallas_call(
            block,
            out_shape=pltpu.VMEM((ROWS, D), bf),
            in_specs=[anywhere] * 4,
            out_specs=vmem,
            scratch_shapes=[
                pltpu.VMEM((ROWS, D), bf),
                pltpu.VMEM((2, D, F), bf),
                pltpu.VMEM((2, ROWS, max(width for width, _ in HIDDEN)), jnp.float32),
                pltpu.VMEM((F, D), bf),
                pltpu.VMEM((ROWS, F), bf),
                chunks(N, jnp.float32),
                chunks(N, bf),
                chunks(N, bf),
                chunks(N, bf),
                chunks(N, bf),
                chunks(2 * max(1, len(DIRECT)), bf),
                dma((1 + sum(len(depths) for _, depths in HIDDEN) + len(DOWN),)),
                dma((len(STEPS),)),
                dma((1 + max(len(groups) for groups in GROUPS),)),
                *[dma] * 4,
            ],
            compiler_params=pltpu.CompilerParams(
                collective_id=0, has_side_effects=True, vmem_limit_bytes=50 * 2**20
            ),
            name="block",
        )(hbm(x), hbm(w_gate), hbm(w_up), hbm(w_down))

    return jax.shard_map(
        step,
        mesh=mesh,
        in_specs=(P("dp", None), P(None, "tp"), P(None, "tp"), P("tp", None)),
        out_specs=P("dp", None),
        check_vma=False,
    )
```

```python
import jax
import jax.numpy as jnp
from jax import lax
from jax.experimental import pallas as pl
from jax.experimental.pallas import tpu as pltpu
from jax.sharding import PartitionSpec as P

ROWS = 128
D = 2048
F = 1536
HIDDEN = ((768, (1024, 1024)), (768, (512, 512, 256, 256, 256, 256)))
DOWN = (256, 256, 512, 1024)
C = 128
N = D // C
STEPS = ((0, 1), (2, 3), (4, 5, 6, 7), (8, 9, 10, 11), (12, 13, 14, 15))
SPLIT = (0, 1)
LAG = ((1, 1, 0, 1, 1), (2, 2, 2, 2, 2))

CUT = {}
GROUPS = (((0, 2, 4, 6), (8, 10)), ((5, 7, 9, 11), (12, 13)))
DIRECT = (1, 3)
SHARED = (14, 15)
MESH = pl.DeviceIdType.MESH
scope = jax.named_scope
OWNER = {k: c for c in range(2) for group in GROUPS[c] for k in group} | {k: 1 for k in DIRECT + SHARED}


def rows(k):
    cut = CUT.get(k % N, ROWS)
    return (0, cut) if k < N else (cut, ROWS - cut)


def stored(k):
    first, n = rows(k)
    return pl.ds((k % N) * ROWS + first, n)


def in_y(k):
    return pl.ds(*rows(k)), pl.ds((k % N) * C, C)


def size(pieces):
    return sum(rows(k)[1] for k in pieces)


def pieces_of(chunks):
    return [k for k in list(chunks) + [N + k for k in chunks if k in CUT]]


def block(x_hbm, wg_hbm, wu_hbm, wd_hbm, out, xv, guv, part, wdv, h, own, tsend, trecv, ssend, srecv, drecv,
          in_sem, t_sem, s_sem, y_sem, send_sem):
    me = lax.axis_index("tp")
    core = lax.rem(me, 2)
    sib = me + 1 - 2 * core
    opp = lax.rem(me + 2, 4)
    cross = 3 - me
    f32 = jnp.float32

    barrier = pltpu.get_barrier_semaphore()
    for other in (sib, opp, cross):
        pl.semaphore_signal(barrier, inc=1, device_id={"tp": other}, device_id_type=MESH)

    loads = []

    def load(ref, *pairs):
        loads.append((ref, pairs))
        return len(loads) - 1

    def start(i):
        for src, dst in loads[i][1]:
            pltpu.make_async_copy(src, dst, in_sem.at[i]).start()

    def loaded(i):
        ref = loads[i][0]
        pltpu.make_async_copy(ref, ref, in_sem.at[i]).wait()

    x_copy = load(xv, (x_hbm, xv))
    hidden, at = [], 0
    for width, depths in HIDDEN:
        cols, top, pieces = pl.ds(at, width), 0, []
        for depth in depths:
            deep = pl.ds(top, depth)
            n = load(
                guv.at[:, deep, cols],
                (wg_hbm.at[deep, cols], guv.at[0, deep, cols]),
                (wu_hbm.at[deep, cols], guv.at[1, deep, cols]),
            )
            pieces.append((n, top, depth))
            top += depth
        hidden.append((at, width, pieces))
        at += width
    down, at = {}, 0
    for width in DOWN:
        cols = pl.ds(at, width)
        down[at // C] = load(wdv.at[:, cols], (wd_hbm.at[:, cols], wdv.at[:, cols]))
        at += width
    for i in range(len(loads)):
        start(i)

    with scope("wait_x"):
        loaded(x_copy)
    for c, (at, width, pieces) in enumerate(hidden):
        cols = slice(at, at + width)
        for n, top, depth in pieces:
            with scope(f"wait_g{c}_{top}"):
                loaded(n)
            with scope(f"hid{c}_{top}"):
                deep = slice(top, top + depth)
                gate = jnp.dot(xv[:, deep], guv[0, deep, cols], preferred_element_type=f32)
                up = jnp.dot(xv[:, deep], guv[1, deep, cols], preferred_element_type=f32)
                if top > 0:
                    gate, up = gate + part[0, :, :width], up + part[1, :, :width]
                if top + depth < D:
                    part[0, :, :width], part[1, :, :width] = gate, up
                else:
                    h[:, cols] = (jax.nn.silu(gate) * up).astype(jnp.bfloat16)
    def remote(src, dst, recv, to):
        return pltpu.make_async_remote_copy(
            src_ref=src, dst_ref=dst, send_sem=send_sem, recv_sem=recv, device_id={"tp": to}, device_id_type=MESH
        )

    def some(n):
        return tsend.at[pl.ds(0, n)], trecv.at[pl.ds(0, n)]

    def wait_recv(sem, n):
        remote(*some(n), sem, sib).wait_recv()

    group_of = {k: g for c in range(2) for g, group in enumerate(GROUPS[c]) for k in group}
    shared_sem = s_sem.at[max(len(groups) for groups in GROUPS)]
    t_slot = lambda j, c: t_sem.at[j - min(i for i in range(len(STEPS)) if summed(i, c))]
    s_copy = lambda k, to: remote(
        ssend.at[stored(k)], srecv.at[stored(k)], shared_sem if k in SHARED else s_sem.at[group_of[k]], to
    )
    d_sem = t_sem.at[len(STEPS) - 2]
    sent = {0: 0, 1: 0}

    def summed(j, c):
        return [k for k in pieces_of(STEPS[j]) if OWNER[k] == c and k not in DIRECT]

    def term(j):
        chunks = STEPS[j]
        if chunks[0] in down:
            with scope(f"wait_d{j}"):
                loaded(down[chunks[0]])
        with scope(f"down{j}"):
            cols = slice(chunks[0] * C, (chunks[-1] + 1) * C)
            if j in SPLIT:
                width = len(chunks) * C
                half = [slice(0, F // 2), slice(F // 2, F)]
                part[me // 4, :, :width] = jnp.dot(h[:, half[0]], wdv[half[0], cols], preferred_element_type=f32)
                value = jnp.dot(h[:, half[1]], wdv[half[1], cols], preferred_element_type=f32) + part[0, :, :width]
            else:
                value = jnp.dot(h[...], wdv[:, cols], preferred_element_type=f32)
            for i, k in enumerate(chunks):
                at = slice(k * ROWS, (k + 1) * ROWS)
                own[at] = value[:, i * C : (i + 1) * C]
                tsend[at] = value[:, i * C : (i + 1) * C].astype(jnp.bfloat16)
            if j == 0:
                pl.semaphore_wait(barrier, 3)
            pieces = pieces_of(chunks)
            for c in range(2):

                @pl.when(core == c)
                def _(c=c):
                    for k in pieces:
                        if k in DIRECT:
                            place = drecv.at[c, stored(k)]
                            remote(tsend.at[stored(k)], place, d_sem, opp if c == OWNER[k] else cross).start()
                            sent[c] += size([k])
                    for k in pieces:
                        if OWNER[k] != c:
                            sem = d_sem if k in DIRECT else t_slot(j, OWNER[k])
                            remote(tsend.at[stored(k)], trecv.at[stored(k)], sem, sib).start()
                            sent[c] += size([k])

    def chip_sum(j, c):
        pieces = summed(j, c)
        if not pieces:
            return
        sent[c] += size(pieces) + 2 * size([k for k in pieces if k in SHARED])

        @pl.when(core == c)
        def _():
            with scope(f"wait_t{j}"):
                wait_recv(t_slot(j, c), size(pieces))
            for k in pieces:
                with scope(f"sum{k}"):
                    at = stored(k)
                    ssend[at] = (own[at] + trecv[at].astype(f32)).astype(jnp.bfloat16)
                    if k in SHARED:
                        s_copy(k, cross).start()
                        remote(ssend.at[at], ssend.at[at], shared_sem, sib).start()
                    else:
                        s_copy(k, opp).start()
            for k in pieces:
                if k in SHARED:
                    s_copy(k, opp).start()

    for j in range(len(STEPS) + 3):
        if j < len(STEPS):
            term(j)
        for c in range(2):
            for k in range(len(STEPS)):
                if k + LAG[c][k] == j:
                    chip_sum(k, c)

    for c in range(2):

        @pl.when(core == c)
        def _(c=c):
            def finish(k, here, there):
                with scope(f"fin{k}"):
                    out[in_y(k)] = (here + there).astype(jnp.bfloat16)
                    if k not in SHARED:
                        place = out.at[in_y(k)]
                        remote(place, place, y_sem, sib).start()
                        sent[c] += size([k])

            if c == 1 and DIRECT:
                with scope("wait_direct"):
                    wait_recv(d_sem, 3 * size(DIRECT))
                for k in DIRECT:
                    at = stored(k)
                    here = tsend[at].astype(f32) + trecv[at].astype(f32)
                    finish(k, here, drecv[1, at].astype(f32) + drecv[0, at].astype(f32))
            for g, group in enumerate(GROUPS[c]):
                with scope(f"wait_s{group[0]}"):
                    wait_recv(s_sem.at[g], size(group))
                for k in group:
                    finish(k, ssend[stored(k)].astype(f32), srecv[stored(k)].astype(f32))
            if SHARED:
                with scope("wait_shared"):
                    wait_recv(shared_sem, size(SHARED) * (2 - c))
            for k in SHARED:
                finish(k, ssend[stored(k)].astype(f32), srecv[stored(k)].astype(f32))
            with scope("drain_send"):
                total = sent[c]
                while total:
                    n = min(total, N * ROWS)
                    remote(*some(n), y_sem, sib).wait_send()
                    total -= n
            with scope("drain_y"):
                wait_recv(y_sem, size([k for k in OWNER if OWNER[k] != c and k not in SHARED]))


def solution(mesh):
    bf = jnp.bfloat16
    dma = pltpu.SemaphoreType.DMA
    anywhere = pl.BlockSpec(memory_space=pl.ANY)
    vmem = pl.BlockSpec(memory_space=pltpu.VMEM)

    def step(x, w_gate, w_up, w_down):
        hbm = lambda a: pltpu.with_memory_space_constraint(a, pltpu.HBM)
        chunks = lambda dtype: pltpu.VMEM((N * ROWS, C), dtype)
        return pl.pallas_call(
            block,
            out_shape=pltpu.VMEM((ROWS, D), bf),
            in_specs=[anywhere] * 4,
            out_specs=vmem,
            scratch_shapes=[
                pltpu.VMEM((ROWS, D), bf),
                pltpu.VMEM((2, D, F), bf),
                pltpu.VMEM((2, ROWS, max(width for width, _ in HIDDEN)), jnp.float32),
                pltpu.VMEM((F, D), bf),
                pltpu.VMEM((ROWS, F), bf),
                chunks(jnp.float32),
                chunks(bf),
                chunks(bf),
                chunks(bf),
                chunks(bf),
                pltpu.VMEM((2, N * ROWS, C), bf),
                dma((1 + sum(len(depths) for _, depths in HIDDEN) + len(DOWN),)),
                dma((len(STEPS) - 1,)),
                dma((1 + max(len(groups) for groups in GROUPS),)),
                *[dma] * 2,
            ],
            compiler_params=pltpu.CompilerParams(
                collective_id=0, has_side_effects=True, vmem_limit_bytes=50 * 2**20
            ),
            name="block",
        )(hbm(x), hbm(w_gate), hbm(w_up), hbm(w_down))

    return jax.shard_map(
        step,
        mesh=mesh,
        in_specs=(P("dp", None), P(None, "tp"), P(None, "tp"), P("tp", None)),
        out_specs=P("dp", None),
        check_vma=False,
    )
```

```python
import jax
import jax.numpy as jnp
from jax import lax
from jax.experimental import pallas as pl
from jax.experimental.pallas import tpu as pltpu
from jax.sharding import PartitionSpec as P

ROWS = 128
D = 2048
F = 1536
HIDDEN = ((768, (1024, 1024)), (768, (512, 512, 256, 256, 256, 256)))
DOWN = (256, 256, 512, 1024)
STEPS = ((0, 1), (2, 3), (4, 5, 6, 7), (8, 9, 10, 11), (12, 13, 14, 15))
LENT = 4
C = 128
N = D // C
SPLIT = (0, 1)
LAG = ((1, 1, 0, 1, 1), (2, 2, 2, 2, 2))

CUT = {}
GROUPS = (((0, 2, 4, 6), (8, 10)), ((5, 7, 9, 11), (12, 13)))
DIRECT = (1, 3)
SHARED = (14, 15)
MESH = pl.DeviceIdType.MESH
scope = jax.named_scope
OWNER = {k: c for c in range(2) for group in GROUPS[c] for k in group} | {k: 1 for k in DIRECT + SHARED}


def rows(k):
    cut = CUT.get(k % N, ROWS)
    return (0, cut) if k < N else (cut, ROWS - cut)


def stored(k):
    first, n = rows(k)
    return pl.ds((k % N) * ROWS + first, n)


def in_y(k):
    return pl.ds(*rows(k)), pl.ds((k % N) * C, C)


def size(pieces):
    return sum(rows(k)[1] for k in pieces)


def pieces_of(chunks):
    return [k for k in list(chunks) + [N + k for k in chunks if k in CUT]]


def block(x_hbm, wg_hbm, wu_hbm, wd_hbm, out, xv, guv, part, wdv, h, own, tsend, trecv, ssend, srecv, drecv,
          in_sem, s_sem):
    me = lax.axis_index("tp")
    core = lax.rem(me, 2)
    sib = me + 1 - 2 * core
    opp = lax.rem(me + 2, 4)
    cross = 3 - me
    f32 = jnp.float32
    n_in = 1 + sum(len(depths) for _, depths in HIDDEN) + len(DOWN)
    t_sem, y_sem, send_sem = in_sem, in_sem.at[n_in], in_sem.at[LENT]

    barrier = pltpu.get_barrier_semaphore()

    def announce():
        for other in (sib, opp, cross):
            pl.semaphore_signal(barrier, inc=1, device_id={"tp": other}, device_id_type=MESH)

    loads = []

    def load(ref, *pairs):
        loads.append((ref, pairs))
        return len(loads) - 1

    def start(i):
        for src, dst in loads[i][1]:
            pltpu.make_async_copy(src, dst, in_sem.at[i]).start()

    def loaded(i):
        ref = loads[i][0]
        pltpu.make_async_copy(ref, ref, in_sem.at[i]).wait()

    x_copy = load(xv, (x_hbm, xv))
    hidden, at = [], 0
    for width, depths in HIDDEN:
        cols, top, pieces = pl.ds(at, width), 0, []
        for depth in depths:
            deep = pl.ds(top, depth)
            n = load(
                guv.at[:, deep, cols],
                (wg_hbm.at[deep, cols], guv.at[0, deep, cols]),
                (wu_hbm.at[deep, cols], guv.at[1, deep, cols]),
            )
            pieces.append((n, top, depth))
            top += depth
        hidden.append((at, width, pieces))
        at += width
    down, at = {}, 0
    for width in DOWN:
        cols = pl.ds(at, width)
        down[at // C] = load(wdv.at[:, cols], (wd_hbm.at[:, cols], wdv.at[:, cols]))
        at += width
    for i in range(len(loads)):
        start(i)

    with scope("wait_x"):
        loaded(x_copy)
    for c, (at, width, pieces) in enumerate(hidden):
        cols = slice(at, at + width)
        for n, top, depth in pieces:
            with scope(f"wait_g{c}_{top}"):
                loaded(n)
            if n == LENT - 1:
                announce()
            with scope(f"hid{c}_{top}"):
                deep = slice(top, top + depth)
                gate = jnp.dot(xv[:, deep], guv[0, deep, cols], preferred_element_type=f32)
                up = jnp.dot(xv[:, deep], guv[1, deep, cols], preferred_element_type=f32)
                if top > 0:
                    gate, up = gate + part[0, :, :width], up + part[1, :, :width]
                if top + depth < D:
                    part[0, :, :width], part[1, :, :width] = gate, up
                else:
                    h[:, cols] = (jax.nn.silu(gate) * up).astype(jnp.bfloat16)
    def remote(src, dst, recv, to):
        return pltpu.make_async_remote_copy(
            src_ref=src, dst_ref=dst, send_sem=send_sem, recv_sem=recv, device_id={"tp": to}, device_id_type=MESH
        )

    def some(n):
        return tsend.at[pl.ds(0, n)], trecv.at[pl.ds(0, n)]

    def wait_recv(sem, n):
        remote(*some(n), sem, sib).wait_recv()

    group_of = {k: g for c in range(2) for g, group in enumerate(GROUPS[c]) for k in group}
    shared_sem = s_sem.at[max(len(groups) for groups in GROUPS)]
    t_slot = lambda j, c: t_sem.at[j - min(i for i in range(len(STEPS)) if summed(i, c))]
    s_copy = lambda k, to: remote(
        ssend.at[stored(k)], srecv.at[stored(k)], shared_sem if k in SHARED else s_sem.at[group_of[k]], to
    )
    d_sem = t_sem.at[len(STEPS) - 2]
    sent = {0: 0, 1: 0}

    def summed(j, c):
        return [k for k in pieces_of(STEPS[j]) if OWNER[k] == c and k not in DIRECT]

    def term(j):
        chunks = STEPS[j]
        if chunks[0] in down:
            with scope(f"wait_d{j}"):
                loaded(down[chunks[0]])
        with scope(f"down{j}"):
            cols = slice(chunks[0] * C, (chunks[-1] + 1) * C)
            if j in SPLIT:
                width = len(chunks) * C
                half = [slice(0, F // 2), slice(F // 2, F)]
                part[me // 4, :, :width] = jnp.dot(h[:, half[0]], wdv[half[0], cols], preferred_element_type=f32)
                value = jnp.dot(h[:, half[1]], wdv[half[1], cols], preferred_element_type=f32) + part[0, :, :width]
            else:
                value = jnp.dot(h[...], wdv[:, cols], preferred_element_type=f32)
            for i, k in enumerate(chunks):
                at = slice(k * ROWS, (k + 1) * ROWS)
                own[at] = value[:, i * C : (i + 1) * C]
                tsend[at] = value[:, i * C : (i + 1) * C].astype(jnp.bfloat16)
            if j == 0:
                pl.semaphore_wait(barrier, 3)
            pieces = pieces_of(chunks)
            for c in range(2):

                @pl.when(core == c)
                def _(c=c):
                    for k in pieces:
                        if k in DIRECT:
                            place = drecv.at[c, stored(k)]
                            remote(tsend.at[stored(k)], place, d_sem, opp if c == OWNER[k] else cross).start()
                            sent[c] += size([k])
                    for k in pieces:
                        if OWNER[k] != c:
                            sem = d_sem if k in DIRECT else t_slot(j, OWNER[k])
                            remote(tsend.at[stored(k)], trecv.at[stored(k)], sem, sib).start()
                            sent[c] += size([k])

    def chip_sum(j, c):
        pieces = summed(j, c)
        if not pieces:
            return
        sent[c] += size(pieces) + 2 * size([k for k in pieces if k in SHARED])

        @pl.when(core == c)
        def _():
            with scope(f"wait_t{j}"):
                wait_recv(t_slot(j, c), size(pieces))
            for k in pieces:
                with scope(f"sum{k}"):
                    at = stored(k)
                    ssend[at] = (own[at] + trecv[at].astype(f32)).astype(jnp.bfloat16)
                    if k in SHARED:
                        s_copy(k, cross).start()
                        remote(ssend.at[at], ssend.at[at], shared_sem, sib).start()
                    else:
                        s_copy(k, opp).start()
            for k in pieces:
                if k in SHARED:
                    s_copy(k, opp).start()

    for j in range(len(STEPS) + 3):
        if j < len(STEPS):
            term(j)
        for c in range(2):
            for k in range(len(STEPS)):
                if k + LAG[c][k] == j:
                    chip_sum(k, c)

    for c in range(2):

        @pl.when(core == c)
        def _(c=c):
            def finish(k, here, there):
                with scope(f"fin{k}"):
                    out[in_y(k)] = (here + there).astype(jnp.bfloat16)
                    if k not in SHARED:
                        place = out.at[in_y(k)]
                        remote(place, place, y_sem, sib).start()
                        sent[c] += size([k])

            if c == 1 and DIRECT:
                with scope("wait_direct"):
                    wait_recv(d_sem, 3 * size(DIRECT))
                for k in DIRECT:
                    at = stored(k)
                    here = tsend[at].astype(f32) + trecv[at].astype(f32)
                    finish(k, here, drecv[1, at].astype(f32) + drecv[0, at].astype(f32))
            for g, group in enumerate(GROUPS[c]):
                with scope(f"wait_s{group[0]}"):
                    wait_recv(s_sem.at[g], size(group))
                for k in group:
                    finish(k, ssend[stored(k)].astype(f32), srecv[stored(k)].astype(f32))
            if SHARED:
                with scope("wait_shared"):
                    wait_recv(shared_sem, size(SHARED) * (2 - c))
            for k in SHARED:
                finish(k, ssend[stored(k)].astype(f32), srecv[stored(k)].astype(f32))
            with scope("drain_send"):
                total = sent[c]
                while total:
                    n = min(total, N * ROWS)
                    remote(*some(n), y_sem, sib).wait_send()
                    total -= n
            with scope("drain_y"):
                wait_recv(y_sem, size([k for k in OWNER if OWNER[k] != c and k not in SHARED]))


def solution(mesh):
    bf = jnp.bfloat16
    dma = pltpu.SemaphoreType.DMA
    anywhere = pl.BlockSpec(memory_space=pl.ANY)
    vmem = pl.BlockSpec(memory_space=pltpu.VMEM)

    def step(x, w_gate, w_up, w_down):
        hbm = lambda a: pltpu.with_memory_space_constraint(a, pltpu.HBM)
        chunks = lambda dtype: pltpu.VMEM((N * ROWS, C), dtype)
        return pl.pallas_call(
            block,
            out_shape=pltpu.VMEM((ROWS, D), bf),
            in_specs=[anywhere] * 4,
            out_specs=vmem,
            scratch_shapes=[
                pltpu.VMEM((ROWS, D), bf),
                pltpu.VMEM((2, D, F), bf),
                pltpu.VMEM((2, ROWS, max(width for width, _ in HIDDEN)), jnp.float32),
                pltpu.VMEM((F, D), bf),
                pltpu.VMEM((ROWS, F), bf),
                chunks(jnp.float32),
                chunks(bf),
                chunks(bf),
                chunks(bf),
                chunks(bf),
                pltpu.VMEM((2, N * ROWS, C), bf),
                dma((2 + sum(len(depths) for _, depths in HIDDEN) + len(DOWN),)),
                dma((1 + max(len(groups) for groups in GROUPS),)),
            ],
            compiler_params=pltpu.CompilerParams(
                collective_id=0, has_side_effects=True, vmem_limit_bytes=50 * 2**20
            ),
            name="block",
        )(hbm(x), hbm(w_gate), hbm(w_up), hbm(w_down))

    return jax.shard_map(
        step,
        mesh=mesh,
        in_specs=(P("dp", None), P(None, "tp"), P(None, "tp"), P("tp", None)),
        out_specs=P("dp", None),
        check_vma=False,
    )
```

```python
import jax
import jax.numpy as jnp
from jax import lax
from jax.experimental import pallas as pl
from jax.experimental.pallas import tpu as pltpu
from jax.sharding import PartitionSpec as P

ROWS = 128
D = 2048
F = 1536
HIDDEN = ((768, (1024, 1024)), (768, (768, 512, 256, 256, 256)))
DOWN = (256, 256, 512, 1024)
STEPS = ((0, 1), (2, 3), (4, 5, 6, 7), (8, 9, 10, 11), (12, 13, 14, 15))
LENT = 4
C = 128
N = D // C
SPLIT = (0, 1)
LAG = ((1, 1, 0, 1, 1), (2, 2, 2, 2, 2))

CUT = {}
GROUPS = (((0, 2, 4, 6), (8, 10)), ((5, 7, 9, 11), (12, 13)))
DIRECT = (1, 3)
SHARED = (14, 15)
MESH = pl.DeviceIdType.MESH
scope = jax.named_scope
OWNER = {k: c for c in range(2) for group in GROUPS[c] for k in group} | {k: 1 for k in DIRECT + SHARED}


def rows(k):
    cut = CUT.get(k % N, ROWS)
    return (0, cut) if k < N else (cut, ROWS - cut)


def stored(k):
    first, n = rows(k)
    return pl.ds((k % N) * ROWS + first, n)


def in_y(k):
    return pl.ds(*rows(k)), pl.ds((k % N) * C, C)


def size(pieces):
    return sum(rows(k)[1] for k in pieces)


def pieces_of(chunks):
    return [k for k in list(chunks) + [N + k for k in chunks if k in CUT]]


def block(x_hbm, wg_hbm, wu_hbm, wd_hbm, out, xv, guv, part, wdv, h, own, tsend, trecv, ssend, srecv, drecv,
          in_sem, s_sem):
    me = lax.axis_index("tp")
    core = lax.rem(me, 2)
    sib = me + 1 - 2 * core
    opp = lax.rem(me + 2, 4)
    cross = 3 - me
    f32 = jnp.float32
    t_sem, send_sem, y_sem = in_sem, in_sem.at[LENT], in_sem.at[LENT + 1]

    barrier = pltpu.get_barrier_semaphore()

    def announce():
        for other in (sib, opp, cross):
            pl.semaphore_signal(barrier, inc=1, device_id={"tp": other}, device_id_type=MESH)

    loads = []

    def load(ref, *pairs):
        loads.append((ref, pairs))
        return len(loads) - 1

    def start(i):
        for src, dst in loads[i][1]:
            pltpu.make_async_copy(src, dst, in_sem.at[i]).start()

    def loaded(i):
        ref = loads[i][0]
        pltpu.make_async_copy(ref, ref, in_sem.at[i]).wait()

    x_copy = load(xv, (x_hbm, xv))
    hidden, at = [], 0
    for width, depths in HIDDEN:
        cols, top, pieces = pl.ds(at, width), 0, []
        for depth in depths:
            deep = pl.ds(top, depth)
            n = load(
                guv.at[:, deep, cols],
                (wg_hbm.at[deep, cols], guv.at[0, deep, cols]),
                (wu_hbm.at[deep, cols], guv.at[1, deep, cols]),
            )
            pieces.append((n, top, depth))
            top += depth
        hidden.append((at, width, pieces))
        at += width
    down, at = {}, 0
    for width in DOWN:
        cols = pl.ds(at, width)
        down[at // C] = load(wdv.at[:, cols], (wd_hbm.at[:, cols], wdv.at[:, cols]))
        at += width
    for i in range(len(loads)):
        start(i)

    with scope("wait_x"):
        loaded(x_copy)
    for c, (at, width, pieces) in enumerate(hidden):
        cols = slice(at, at + width)
        for n, top, depth in pieces:
            with scope(f"wait_g{c}_{top}"):
                loaded(n)
            if n == LENT - 1:
                announce()
            with scope(f"hid{c}_{top}"):
                deep = slice(top, top + depth)
                gate = jnp.dot(xv[:, deep], guv[0, deep, cols], preferred_element_type=f32)
                up = jnp.dot(xv[:, deep], guv[1, deep, cols], preferred_element_type=f32)
                if top > 0:
                    gate, up = gate + part[0, :, :width], up + part[1, :, :width]
                if top + depth < D:
                    part[0, :, :width], part[1, :, :width] = gate, up
                else:
                    h[:, cols] = (jax.nn.silu(gate) * up).astype(jnp.bfloat16)
    def remote(src, dst, recv, to):
        return pltpu.make_async_remote_copy(
            src_ref=src, dst_ref=dst, send_sem=send_sem, recv_sem=recv, device_id={"tp": to}, device_id_type=MESH
        )

    def some(n):
        return tsend.at[pl.ds(0, n)], trecv.at[pl.ds(0, n)]

    def wait_recv(sem, n):
        remote(*some(n), sem, sib).wait_recv()

    group_of = {k: g for c in range(2) for g, group in enumerate(GROUPS[c]) for k in group}
    shared_sem = s_sem.at[max(len(groups) for groups in GROUPS)]
    t_slot = lambda j, c: t_sem.at[j - min(i for i in range(len(STEPS)) if summed(i, c))]
    s_copy = lambda k, to: remote(
        ssend.at[stored(k)], srecv.at[stored(k)], shared_sem if k in SHARED else s_sem.at[group_of[k]], to
    )
    d_sem = t_sem.at[len(STEPS) - 2]
    sent = {0: 0, 1: 0}

    def summed(j, c):
        return [k for k in pieces_of(STEPS[j]) if OWNER[k] == c and k not in DIRECT]

    def term(j):
        chunks = STEPS[j]
        if chunks[0] in down:
            with scope(f"wait_d{j}"):
                loaded(down[chunks[0]])
        with scope(f"down{j}"):
            cols = slice(chunks[0] * C, (chunks[-1] + 1) * C)
            if j in SPLIT:
                width = len(chunks) * C
                half = [slice(0, F // 2), slice(F // 2, F)]
                part[me // 4, :, :width] = jnp.dot(h[:, half[0]], wdv[half[0], cols], preferred_element_type=f32)
                value = jnp.dot(h[:, half[1]], wdv[half[1], cols], preferred_element_type=f32) + part[0, :, :width]
            else:
                value = jnp.dot(h[...], wdv[:, cols], preferred_element_type=f32)
            for i, k in enumerate(chunks):
                at = slice(k * ROWS, (k + 1) * ROWS)
                if k not in DIRECT:
                    own[at] = value[:, i * C : (i + 1) * C]
                tsend[at] = value[:, i * C : (i + 1) * C].astype(jnp.bfloat16)
            if j == 0:
                pl.semaphore_wait(barrier, 3)
            pieces = pieces_of(chunks)
            for c in range(2):

                @pl.when(core == c)
                def _(c=c):
                    for k in pieces:
                        if k in DIRECT:
                            place = drecv.at[c, stored(k)]
                            remote(tsend.at[stored(k)], place, d_sem, opp if c == OWNER[k] else cross).start()
                            sent[c] += size([k])
                    for k in pieces:
                        if OWNER[k] != c:
                            sem = d_sem if k in DIRECT else t_slot(j, OWNER[k])
                            remote(tsend.at[stored(k)], trecv.at[stored(k)], sem, sib).start()
                            sent[c] += size([k])

    def chip_sum(j, c):
        pieces = summed(j, c)
        if not pieces:
            return
        sent[c] += size(pieces) + 2 * size([k for k in pieces if k in SHARED])

        @pl.when(core == c)
        def _():
            with scope(f"wait_t{j}"):
                wait_recv(t_slot(j, c), size(pieces))
            for k in pieces:
                with scope(f"sum{k}"):
                    at = stored(k)
                    ssend[at] = (own[at] + trecv[at].astype(f32)).astype(jnp.bfloat16)
                    if k in SHARED:
                        s_copy(k, cross).start()
                        remote(ssend.at[at], ssend.at[at], shared_sem, sib).start()
                    else:
                        s_copy(k, opp).start()
            for k in pieces:
                if k in SHARED:
                    s_copy(k, opp).start()

    for j in range(len(STEPS) + 3):
        if j < len(STEPS):
            term(j)
        for c in range(2):
            for k in range(len(STEPS)):
                if k + LAG[c][k] == j:
                    chip_sum(k, c)

    for c in range(2):

        @pl.when(core == c)
        def _(c=c):
            def finish(k, here, there):
                with scope(f"fin{k}"):
                    out[in_y(k)] = (here + there).astype(jnp.bfloat16)
                    if k not in SHARED:
                        place = out.at[in_y(k)]
                        remote(place, place, y_sem, sib).start()
                        sent[c] += size([k])

            if c == 1 and DIRECT:
                with scope("wait_direct"):
                    wait_recv(d_sem, 3 * size(DIRECT))
                for k in DIRECT:
                    at = stored(k)
                    here = tsend[at].astype(f32) + trecv[at].astype(f32)
                    finish(k, here, drecv[1, at].astype(f32) + drecv[0, at].astype(f32))
            for g, group in enumerate(GROUPS[c]):
                with scope(f"wait_s{group[0]}"):
                    wait_recv(s_sem.at[g], size(group))
                for k in group:
                    finish(k, ssend[stored(k)].astype(f32), srecv[stored(k)].astype(f32))
            if SHARED:
                with scope("wait_shared"):
                    wait_recv(shared_sem, size(SHARED) * (2 - c))
            for k in SHARED:
                finish(k, ssend[stored(k)].astype(f32), srecv[stored(k)].astype(f32))
            with scope("drain_send"):
                total = sent[c]
                while total:
                    n = min(total, N * ROWS)
                    remote(*some(n), y_sem, sib).wait_send()
                    total -= n
            with scope("drain_y"):
                wait_recv(y_sem, size([k for k in OWNER if OWNER[k] != c and k not in SHARED]))


def solution(mesh):
    bf = jnp.bfloat16
    dma = pltpu.SemaphoreType.DMA
    anywhere = pl.BlockSpec(memory_space=pl.ANY)
    vmem = pl.BlockSpec(memory_space=pltpu.VMEM)

    def step(x, w_gate, w_up, w_down):
        hbm = lambda a: pltpu.with_memory_space_constraint(a, pltpu.HBM)
        chunks = lambda dtype: pltpu.VMEM((N * ROWS, C), dtype)
        return pl.pallas_call(
            block,
            out_shape=pltpu.VMEM((ROWS, D), bf),
            in_specs=[anywhere] * 4,
            out_specs=vmem,
            scratch_shapes=[
                pltpu.VMEM((ROWS, D), bf),
                pltpu.VMEM((2, D, F), bf),
                pltpu.VMEM((2, ROWS, max(width for width, _ in HIDDEN)), jnp.float32),
                pltpu.VMEM((F, D), bf),
                pltpu.VMEM((ROWS, F), bf),
                chunks(jnp.float32),
                chunks(bf),
                chunks(bf),
                chunks(bf),
                chunks(bf),
                pltpu.VMEM((2, N * ROWS, C), bf),
                dma((1 + sum(len(depths) for _, depths in HIDDEN) + len(DOWN),)),
                dma((1 + max(len(groups) for groups in GROUPS),)),
            ],
            compiler_params=pltpu.CompilerParams(
                collective_id=0, has_side_effects=True, vmem_limit_bytes=50 * 2**20
            ),
            name="block",
        )(hbm(x), hbm(w_gate), hbm(w_up), hbm(w_down))

    return jax.shard_map(
        step,
        mesh=mesh,
        in_specs=(P("dp", None), P(None, "tp"), P(None, "tp"), P("tp", None)),
        out_specs=P("dp", None),
        check_vma=False,
    )
```

```python
import jax
import jax.numpy as jnp
from jax import lax
from jax.experimental import pallas as pl
from jax.experimental.pallas import tpu as pltpu
from jax.sharding import PartitionSpec as P

ROWS = 128
D = 2048
F = 1536
HIDDEN = ((768, (1024, 1024)), (768, (768, 512, 256, 256, 256)))
DOWN = (256, 256, 512, 1024)
STEPS = ((0, 1), (2, 3), (4, 5, 6, 7), (8, 9, 10, 11), (12, 13, 14, 15))
LENT = 4
C = 128
N = D // C
SPLIT = (0, 1)
LAG = ((1, 1, 0, 1, 1), (2, 2, 2, 2, 2))

CUT = {}
GROUPS = (((0, 2, 6), (8, 10), (4,)), ((5, 7, 9, 11), (12, 13)))
DIRECT = (1, 3)
SHARED = (14, 15)
DETOUR = 4
RELAY_STEP = 3
SOURCE, RELAY, TARGET, GIVER = ({"dp": d, "tp": t} for d, t in ((0, 2), (1, 3), (0, 1), (0, 0)))
MESH = pl.DeviceIdType.MESH
scope = jax.named_scope
OWNER = {k: c for c in range(2) for group in GROUPS[c] for k in group} | {k: 1 for k in DIRECT + SHARED}


def rows(k):
    cut = CUT.get(k % N, ROWS)
    return (0, cut) if k < N else (cut, ROWS - cut)


def stored(k):
    first, n = rows(k)
    return pl.ds((k % N) * ROWS + first, n)


def in_y(k):
    return pl.ds(*rows(k)), pl.ds((k % N) * C, C)


def size(pieces):
    return sum(rows(k)[1] for k in pieces)


def pieces_of(chunks):
    return [k for k in list(chunks) + [N + k for k in chunks if k in CUT]]


def block(x_hbm, wg_hbm, wu_hbm, wd_hbm, out, xv, guv, part, wdv, h, own, tsend, trecv, ssend, srecv, drecv,
          relayed, in_sem, s_sem, relay_sem):
    me = lax.axis_index("tp")
    dp = lax.axis_index("dp")
    at_place = lambda place: jnp.logical_and(dp == place["dp"], me == place["tp"])
    not_at = lambda place: jnp.logical_or(dp != place["dp"], me != place["tp"])
    core = lax.rem(me, 2)
    sib = me + 1 - 2 * core
    opp = lax.rem(me + 2, 4)
    cross = 3 - me
    f32 = jnp.float32
    t_sem, send_sem, y_sem = in_sem, in_sem.at[LENT], in_sem.at[LENT + 1]

    barrier = pltpu.get_barrier_semaphore()

    def announce():
        for other in (sib, opp, cross):
            pl.semaphore_signal(barrier, inc=1, device_id={"tp": other}, device_id_type=MESH)
        for receiver, sender in ((RELAY, SOURCE), (TARGET, RELAY)):

            @pl.when(at_place(receiver))
            def _(sender=sender):
                pl.semaphore_signal(barrier, inc=1, device_id=sender, device_id_type=MESH)

    loads = []

    def load(ref, *pairs):
        loads.append((ref, pairs))
        return len(loads) - 1

    def start(i):
        for src, dst in loads[i][1]:
            pltpu.make_async_copy(src, dst, in_sem.at[i]).start()

    def loaded(i):
        ref = loads[i][0]
        pltpu.make_async_copy(ref, ref, in_sem.at[i]).wait()

    x_copy = load(xv, (x_hbm, xv))
    hidden, at = [], 0
    for width, depths in HIDDEN:
        cols, top, pieces = pl.ds(at, width), 0, []
        for depth in depths:
            deep = pl.ds(top, depth)
            n = load(
                guv.at[:, deep, cols],
                (wg_hbm.at[deep, cols], guv.at[0, deep, cols]),
                (wu_hbm.at[deep, cols], guv.at[1, deep, cols]),
            )
            pieces.append((n, top, depth))
            top += depth
        hidden.append((at, width, pieces))
        at += width
    down, at = {}, 0
    for width in DOWN:
        cols = pl.ds(at, width)
        down[at // C] = load(wdv.at[:, cols], (wd_hbm.at[:, cols], wdv.at[:, cols]))
        at += width
    for i in range(len(loads)):
        start(i)

    with scope("wait_x"):
        loaded(x_copy)
    for c, (at, width, pieces) in enumerate(hidden):
        cols = slice(at, at + width)
        for n, top, depth in pieces:
            with scope(f"wait_g{c}_{top}"):
                loaded(n)
            if n == LENT - 1:
                announce()
            with scope(f"hid{c}_{top}"):
                deep = slice(top, top + depth)
                gate = jnp.dot(xv[:, deep], guv[0, deep, cols], preferred_element_type=f32)
                up = jnp.dot(xv[:, deep], guv[1, deep, cols], preferred_element_type=f32)
                if top > 0:
                    gate, up = gate + part[0, :, :width], up + part[1, :, :width]
                if top + depth < D:
                    part[0, :, :width], part[1, :, :width] = gate, up
                else:
                    h[:, cols] = (jax.nn.silu(gate) * up).astype(jnp.bfloat16)
    def remote(src, dst, recv, to):
        return pltpu.make_async_remote_copy(
            src_ref=src,
            dst_ref=dst,
            send_sem=send_sem,
            recv_sem=recv,
            device_id=to if isinstance(to, dict) else {"tp": to},
            device_id_type=MESH,
        )

    def some(n):
        return tsend.at[pl.ds(0, n)], trecv.at[pl.ds(0, n)]

    def wait_recv(sem, n):
        remote(*some(n), sem, sib).wait_recv()

    group_of = {k: g for c in range(2) for g, group in enumerate(GROUPS[c]) for k in group}
    shared_sem = s_sem.at[max(len(groups) for groups in GROUPS)]
    t_slot = lambda j, c: t_sem.at[j - min(i for i in range(len(STEPS)) if summed(i, c))]
    s_copy = lambda k, to: remote(
        ssend.at[stored(k)], srecv.at[stored(k)], shared_sem if k in SHARED else s_sem.at[group_of[k]], to
    )
    d_sem = t_sem.at[len(STEPS) - 2]
    sent = {0: 0, 1: 0}

    def summed(j, c):
        return [k for k in pieces_of(STEPS[j]) if OWNER[k] == c and k not in DIRECT]

    def term(j):
        chunks = STEPS[j]
        if chunks[0] in down:
            with scope(f"wait_d{j}"):
                loaded(down[chunks[0]])
        with scope(f"down{j}"):
            cols = slice(chunks[0] * C, (chunks[-1] + 1) * C)
            if j in SPLIT:
                width = len(chunks) * C
                half = [slice(0, F // 2), slice(F // 2, F)]
                part[me // 4, :, :width] = jnp.dot(h[:, half[0]], wdv[half[0], cols], preferred_element_type=f32)
                value = jnp.dot(h[:, half[1]], wdv[half[1], cols], preferred_element_type=f32) + part[0, :, :width]
            else:
                value = jnp.dot(h[...], wdv[:, cols], preferred_element_type=f32)
            for i, k in enumerate(chunks):
                at = slice(k * ROWS, (k + 1) * ROWS)
                if k not in DIRECT:
                    own[at] = value[:, i * C : (i + 1) * C]
                tsend[at] = value[:, i * C : (i + 1) * C].astype(jnp.bfloat16)
            if j == 0:
                more = jnp.logical_or(at_place(SOURCE), at_place(RELAY)).astype(jnp.int32)
                pl.semaphore_wait(barrier, 3 + more)
            pieces = pieces_of(chunks)
            for c in range(2):

                @pl.when(core == c)
                def _(c=c):
                    for k in pieces:
                        if k in DIRECT:
                            place = drecv.at[c, stored(k)]
                            remote(tsend.at[stored(k)], place, d_sem, opp if c == OWNER[k] else cross).start()
                            sent[c] += size([k])
                    for k in pieces:
                        if OWNER[k] != c:
                            sem = d_sem if k in DIRECT else t_slot(j, OWNER[k])
                            remote(tsend.at[stored(k)], trecv.at[stored(k)], sem, sib).start()
                            sent[c] += size([k])

    def chip_sum(j, c):
        pieces = summed(j, c)
        if not pieces:
            return
        sent[c] += size(pieces) + 2 * size([k for k in pieces if k in SHARED])

        @pl.when(core == c)
        def _():
            if c == 1 and j == RELAY_STEP:

                @pl.when(at_place(RELAY))
                def _():
                    with scope("relay"):
                        wait_recv(relay_sem, size([DETOUR]))
                        remote(relayed, srecv.at[stored(DETOUR)], s_sem.at[group_of[DETOUR]], TARGET).start()

            with scope(f"wait_t{j}"):
                wait_recv(t_slot(j, c), size(pieces))
            for k in pieces:
                with scope(f"sum{k}"):
                    at = stored(k)
                    ssend[at] = (own[at] + trecv[at].astype(f32)).astype(jnp.bfloat16)
                    if k in SHARED:
                        s_copy(k, cross).start()
                        remote(ssend.at[at], ssend.at[at], shared_sem, sib).start()
                    elif k == DETOUR:

                        @pl.when(at_place(SOURCE))
                        def _(at=at):
                            remote(ssend.at[at], relayed, relay_sem, RELAY).start()

                        @pl.when(not_at(SOURCE))
                        def _(k=k):
                            s_copy(k, opp).start()

                        @pl.when(at_place(GIVER))
                        def _(at=at):
                            remote(ssend.at[at], ssend.at[at], relay_sem, sib).start()

                    else:
                        s_copy(k, opp).start()
            for k in pieces:
                if k in SHARED:
                    s_copy(k, opp).start()

    for j in range(len(STEPS) + 3):
        if j < len(STEPS):
            term(j)
        for c in range(2):
            for k in range(len(STEPS)):
                if k + LAG[c][k] == j:
                    chip_sum(k, c)

    for c in range(2):

        @pl.when(core == c)
        def _(c=c):
            def finish(k, here, there):
                with scope(f"fin{k}"):
                    out[in_y(k)] = (here + there).astype(jnp.bfloat16)
                    if k not in SHARED:
                        place = out.at[in_y(k)]
                        remote(place, place, y_sem, sib).start()
                        sent[c] += size([k])

            if c == 1 and DIRECT:
                with scope("wait_direct"):
                    wait_recv(d_sem, 3 * size(DIRECT))
                for k in DIRECT:
                    at = stored(k)
                    here = tsend[at].astype(f32) + trecv[at].astype(f32)
                    finish(k, here, drecv[1, at].astype(f32) + drecv[0, at].astype(f32))
            def finish_group(g, group):
                with scope(f"wait_s{group[0]}"):
                    wait_recv(s_sem.at[g], size(group))
                for k in group:
                    finish(k, ssend[stored(k)].astype(f32), srecv[stored(k)].astype(f32))

            for g, group in enumerate(GROUPS[c]):
                if DETOUR in group:
                    pl.when(not_at(GIVER))(lambda g=g, group=group: finish_group(g, group))
                else:
                    finish_group(g, group)
                if c == 1 and g == 0:

                    @pl.when(at_place(TARGET))
                    def _():
                        wait_recv(relay_sem, size([DETOUR]))
                        finish_group(group_of[DETOUR], [DETOUR])
                        sent[c] -= size([DETOUR])

            if SHARED:
                with scope("wait_shared"):
                    wait_recv(shared_sem, size(SHARED) * (2 - c))
            for k in SHARED:
                finish(k, ssend[stored(k)].astype(f32), srecv[stored(k)].astype(f32))
            with scope("drain"):
                come = size([k for k in OWNER if OWNER[k] != c and k not in SHARED])
                more = size([DETOUR])
                cases = [(at_place(GIVER), 0, more)] if c == 0 else [(at_place(TARGET), more, -more), (at_place(RELAY), more, 0)]
                cases.append((not_at(GIVER) if c == 0 else jnp.logical_and(not_at(TARGET), not_at(RELAY)), 0, 0))
                for place, extra_sent, extra_come in cases:

                    @pl.when(place)
                    def _(extra_sent=extra_sent, extra_come=extra_come):
                        total = sent[c] + extra_sent
                        while total:
                            n = min(total, N * ROWS)
                            remote(*some(n), y_sem, sib).wait_send()
                            total -= n
                        wait_recv(y_sem, come + extra_come)


def solution(mesh):
    bf = jnp.bfloat16
    dma = pltpu.SemaphoreType.DMA
    anywhere = pl.BlockSpec(memory_space=pl.ANY)
    vmem = pl.BlockSpec(memory_space=pltpu.VMEM)

    def step(x, w_gate, w_up, w_down):
        hbm = lambda a: pltpu.with_memory_space_constraint(a, pltpu.HBM)
        chunks = lambda dtype: pltpu.VMEM((N * ROWS, C), dtype)
        return pl.pallas_call(
            block,
            out_shape=pltpu.VMEM((ROWS, D), bf),
            in_specs=[anywhere] * 4,
            out_specs=vmem,
            scratch_shapes=[
                pltpu.VMEM((ROWS, D), bf),
                pltpu.VMEM((2, D, F), bf),
                pltpu.VMEM((2, ROWS, max(width for width, _ in HIDDEN)), jnp.float32),
                pltpu.VMEM((F, D), bf),
                pltpu.VMEM((ROWS, F), bf),
                chunks(jnp.float32),
                chunks(bf),
                chunks(bf),
                chunks(bf),
                chunks(bf),
                pltpu.VMEM((2, N * ROWS, C), bf),
                pltpu.VMEM((ROWS, C), bf),
                dma((1 + sum(len(depths) for _, depths in HIDDEN) + len(DOWN),)),
                dma((1 + max(len(groups) for groups in GROUPS),)),
                dma,
            ],
            compiler_params=pltpu.CompilerParams(
                collective_id=0, has_side_effects=True, vmem_limit_bytes=50 * 2**20
            ),
            name="block",
        )(hbm(x), hbm(w_gate), hbm(w_up), hbm(w_down))

    return jax.shard_map(
        step,
        mesh=mesh,
        in_specs=(P("dp", None), P(None, "tp"), P(None, "tp"), P("tp", None)),
        out_specs=P("dp", None),
        check_vma=False,
    )
```

```python
import jax
import jax.numpy as jnp
from jax import lax
from jax.experimental import pallas as pl
from jax.experimental.pallas import tpu as pltpu
from jax.sharding import PartitionSpec as P

ROWS = 128
D = 2048
F = 1536
HIDDEN = ((768, (1024, 1024)), (768, (768, 512, 256, 256, 256)))
DOWN = (256, 256, 512, 1024)
STEPS = ((0, 1), (2, 3), (4, 5, 6, 7), (8, 9, 10, 11), (12, 13, 14, 15))
LENT = 4
C = 128
N = D // C
SPLIT = (0, 1)
LAG = ((1, 1, 0, 1, 1), (2, 2, 2, 2, 2))

CUT = {4: 48}
GROUPS = (((0, 2, 6), (8, 10), (4, 20)), ((5, 7, 9, 11), (12, 13)))
DIRECT = (1, 3)
SHARED = (14, 15)
DETOUR = (4, 20)
RELAY_STEP = 3
SOURCE, RELAY, TARGET, GIVER = ({"dp": d, "tp": t} for d, t in ((0, 2), (1, 3), (0, 1), (0, 0)))
MESH = pl.DeviceIdType.MESH
scope = jax.named_scope
OWNER = {k: c for c in range(2) for group in GROUPS[c] for k in group} | {k: 1 for k in DIRECT + SHARED}


def rows(k):
    cut = CUT.get(k % N, ROWS)
    return (0, cut) if k < N else (cut, ROWS - cut)


def stored(k):
    first, n = rows(k)
    return pl.ds((k % N) * ROWS + first, n)


def in_y(k):
    return pl.ds(*rows(k)), pl.ds((k % N) * C, C)


def size(pieces):
    return sum(rows(k)[1] for k in pieces)


def pieces_of(chunks):
    return [k for k in list(chunks) + [N + k for k in chunks if k in CUT]]


def block(x_hbm, wg_hbm, wu_hbm, wd_hbm, out, xv, guv, part, wdv, h, own, tsend, trecv, ssend, srecv, drecv,
          relayed, in_sem, s_sem, relay_sem):
    me = lax.axis_index("tp")
    dp = lax.axis_index("dp")
    at_place = lambda place: jnp.logical_and(dp == place["dp"], me == place["tp"])
    not_at = lambda place: jnp.logical_or(dp != place["dp"], me != place["tp"])
    core = lax.rem(me, 2)
    sib = me + 1 - 2 * core
    opp = lax.rem(me + 2, 4)
    cross = 3 - me
    f32 = jnp.float32
    t_sem, send_sem, y_sem = in_sem, in_sem.at[LENT], in_sem.at[LENT + 1]

    barrier = pltpu.get_barrier_semaphore()

    def announce():
        for other in (sib, opp, cross):
            pl.semaphore_signal(barrier, inc=1, device_id={"tp": other}, device_id_type=MESH)
        for receiver, sender in ((RELAY, SOURCE), (TARGET, RELAY)):

            @pl.when(at_place(receiver))
            def _(sender=sender):
                pl.semaphore_signal(barrier, inc=1, device_id=sender, device_id_type=MESH)

    loads = []

    def load(ref, *pairs):
        loads.append((ref, pairs))
        return len(loads) - 1

    def start(i):
        for src, dst in loads[i][1]:
            pltpu.make_async_copy(src, dst, in_sem.at[i]).start()

    def loaded(i):
        ref = loads[i][0]
        pltpu.make_async_copy(ref, ref, in_sem.at[i]).wait()

    x_copy = load(xv, (x_hbm, xv))
    hidden, at = [], 0
    for width, depths in HIDDEN:
        cols, top, pieces = pl.ds(at, width), 0, []
        for depth in depths:
            deep = pl.ds(top, depth)
            n = load(
                guv.at[:, deep, cols],
                (wg_hbm.at[deep, cols], guv.at[0, deep, cols]),
                (wu_hbm.at[deep, cols], guv.at[1, deep, cols]),
            )
            pieces.append((n, top, depth))
            top += depth
        hidden.append((at, width, pieces))
        at += width
    down, at = {}, 0
    for width in DOWN:
        cols = pl.ds(at, width)
        down[at // C] = load(wdv.at[:, cols], (wd_hbm.at[:, cols], wdv.at[:, cols]))
        at += width
    for i in range(len(loads)):
        start(i)

    with scope("wait_x"):
        loaded(x_copy)
    for c, (at, width, pieces) in enumerate(hidden):
        cols = slice(at, at + width)
        for n, top, depth in pieces:
            with scope(f"wait_g{c}_{top}"):
                loaded(n)
            if n == LENT - 1:
                announce()
            with scope(f"hid{c}_{top}"):
                deep = slice(top, top + depth)
                gate = jnp.dot(xv[:, deep], guv[0, deep, cols], preferred_element_type=f32)
                up = jnp.dot(xv[:, deep], guv[1, deep, cols], preferred_element_type=f32)
                if top > 0:
                    gate, up = gate + part[0, :, :width], up + part[1, :, :width]
                if top + depth < D:
                    part[0, :, :width], part[1, :, :width] = gate, up
                else:
                    h[:, cols] = (jax.nn.silu(gate) * up).astype(jnp.bfloat16)
    def remote(src, dst, recv, to):
        return pltpu.make_async_remote_copy(
            src_ref=src,
            dst_ref=dst,
            send_sem=send_sem,
            recv_sem=recv,
            device_id=to if isinstance(to, dict) else {"tp": to},
            device_id_type=MESH,
        )

    def some(n):
        return tsend.at[pl.ds(0, n)], trecv.at[pl.ds(0, n)]

    def wait_recv(sem, n):
        remote(*some(n), sem, sib).wait_recv()

    group_of = {k: g for c in range(2) for g, group in enumerate(GROUPS[c]) for k in group}
    shared_sem = s_sem.at[max(len(groups) for groups in GROUPS)]
    t_slot = lambda j, c: t_sem.at[j - min(i for i in range(len(STEPS)) if summed(i, c))]
    s_copy = lambda k, to: remote(
        ssend.at[stored(k)], srecv.at[stored(k)], shared_sem if k in SHARED else s_sem.at[group_of[k]], to
    )
    d_sem = t_sem.at[len(STEPS) - 2]
    sent = {0: 0, 1: 0}

    def summed(j, c):
        return [k for k in pieces_of(STEPS[j]) if OWNER[k] == c and k not in DIRECT]

    def term(j):
        chunks = STEPS[j]
        if chunks[0] in down:
            with scope(f"wait_d{j}"):
                loaded(down[chunks[0]])
        with scope(f"down{j}"):
            cols = slice(chunks[0] * C, (chunks[-1] + 1) * C)
            if j in SPLIT:
                width = len(chunks) * C
                half = [slice(0, F // 2), slice(F // 2, F)]
                part[me // 4, :, :width] = jnp.dot(h[:, half[0]], wdv[half[0], cols], preferred_element_type=f32)
                value = jnp.dot(h[:, half[1]], wdv[half[1], cols], preferred_element_type=f32) + part[0, :, :width]
            else:
                value = jnp.dot(h[...], wdv[:, cols], preferred_element_type=f32)
            for i, k in enumerate(chunks):
                at = slice(k * ROWS, (k + 1) * ROWS)
                if k not in DIRECT:
                    own[at] = value[:, i * C : (i + 1) * C]
                tsend[at] = value[:, i * C : (i + 1) * C].astype(jnp.bfloat16)
            if j == 0:
                more = jnp.logical_or(at_place(SOURCE), at_place(RELAY)).astype(jnp.int32)
                pl.semaphore_wait(barrier, 3 + more)
            pieces = pieces_of(chunks)
            for c in range(2):

                @pl.when(core == c)
                def _(c=c):
                    for k in pieces:
                        if k in DIRECT:
                            place = drecv.at[c, stored(k)]
                            remote(tsend.at[stored(k)], place, d_sem, opp if c == OWNER[k] else cross).start()
                            sent[c] += size([k])
                    for k in pieces:
                        if OWNER[k] != c:
                            sem = d_sem if k in DIRECT else t_slot(j, OWNER[k])
                            remote(tsend.at[stored(k)], trecv.at[stored(k)], sem, sib).start()
                            sent[c] += size([k])

    def chip_sum(j, c):
        pieces = summed(j, c)
        if not pieces:
            return
        sent[c] += size(pieces) + 2 * size([k for k in pieces if k in SHARED])

        @pl.when(core == c)
        def _():
            if c == 1 and j == RELAY_STEP:

                @pl.when(at_place(RELAY))
                def _():
                    with scope("relay"):
                        for i, k in enumerate(DETOUR):
                            wait_recv(relay_sem.at[i], size([k]))
                            place = srecv.at[stored(k)]
                            remote(relayed.at[pl.ds(*rows(k))], place, s_sem.at[group_of[k]], TARGET).start()

            with scope(f"wait_t{j}"):
                wait_recv(t_slot(j, c), size(pieces))
            for k in pieces:
                with scope(f"sum{k}"):
                    at = stored(k)
                    ssend[at] = (own[at] + trecv[at].astype(f32)).astype(jnp.bfloat16)
                    if k in SHARED:
                        s_copy(k, cross).start()
                        remote(ssend.at[at], ssend.at[at], shared_sem, sib).start()
                    elif k in DETOUR:

                        @pl.when(at_place(SOURCE))
                        def _(k=k, at=at):
                            place = relayed.at[pl.ds(*rows(k))]
                            remote(ssend.at[at], place, relay_sem.at[DETOUR.index(k)], RELAY).start()

                        @pl.when(not_at(SOURCE))
                        def _(k=k):
                            s_copy(k, opp).start()

                        @pl.when(at_place(GIVER))
                        def _(at=at):
                            remote(ssend.at[at], ssend.at[at], relay_sem.at[0], sib).start()

                    else:
                        s_copy(k, opp).start()
            for k in pieces:
                if k in SHARED:
                    s_copy(k, opp).start()

    for j in range(len(STEPS) + 3):
        if j < len(STEPS):
            term(j)
        for c in range(2):
            for k in range(len(STEPS)):
                if k + LAG[c][k] == j:
                    chip_sum(k, c)

    for c in range(2):

        @pl.when(core == c)
        def _(c=c):
            def finish(k, here, there):
                with scope(f"fin{k}"):
                    out[in_y(k)] = (here + there).astype(jnp.bfloat16)
                    if k not in SHARED:
                        place = out.at[in_y(k)]
                        remote(place, place, y_sem, sib).start()
                        sent[c] += size([k])

            if c == 1 and DIRECT:
                with scope("wait_direct"):
                    wait_recv(d_sem, 3 * size(DIRECT))
                for k in DIRECT:
                    at = stored(k)
                    here = tsend[at].astype(f32) + trecv[at].astype(f32)
                    finish(k, here, drecv[1, at].astype(f32) + drecv[0, at].astype(f32))
            def finish_group(g, group):
                with scope(f"wait_s{group[0]}"):
                    wait_recv(s_sem.at[g], size(group))
                for k in group:
                    finish(k, ssend[stored(k)].astype(f32), srecv[stored(k)].astype(f32))

            for g, group in enumerate(GROUPS[c]):
                if DETOUR == group:
                    pl.when(not_at(GIVER))(lambda g=g, group=group: finish_group(g, group))
                else:
                    finish_group(g, group)
                if c == 1 and g == 0:

                    @pl.when(at_place(TARGET))
                    def _():
                        wait_recv(relay_sem.at[0], size(DETOUR))
                        finish_group(group_of[DETOUR[0]], DETOUR)
                        sent[c] -= size(DETOUR)

            if SHARED:
                with scope("wait_shared"):
                    wait_recv(shared_sem, size(SHARED) * (2 - c))
            for k in SHARED:
                finish(k, ssend[stored(k)].astype(f32), srecv[stored(k)].astype(f32))
            with scope("drain"):
                come = size([k for k in OWNER if OWNER[k] != c and k not in SHARED])
                more = size(DETOUR)
                cases = [(at_place(GIVER), 0, more)] if c == 0 else [(at_place(TARGET), more, -more), (at_place(RELAY), more, 0)]
                cases.append((not_at(GIVER) if c == 0 else jnp.logical_and(not_at(TARGET), not_at(RELAY)), 0, 0))
                for place, extra_sent, extra_come in cases:

                    @pl.when(place)
                    def _(extra_sent=extra_sent, extra_come=extra_come):
                        total = sent[c] + extra_sent
                        while total:
                            n = min(total, N * ROWS)
                            remote(*some(n), y_sem, sib).wait_send()
                            total -= n
                        wait_recv(y_sem, come + extra_come)


def solution(mesh):
    bf = jnp.bfloat16
    dma = pltpu.SemaphoreType.DMA
    anywhere = pl.BlockSpec(memory_space=pl.ANY)
    vmem = pl.BlockSpec(memory_space=pltpu.VMEM)

    def step(x, w_gate, w_up, w_down):
        hbm = lambda a: pltpu.with_memory_space_constraint(a, pltpu.HBM)
        chunks = lambda dtype: pltpu.VMEM((N * ROWS, C), dtype)
        return pl.pallas_call(
            block,
            out_shape=pltpu.VMEM((ROWS, D), bf),
            in_specs=[anywhere] * 4,
            out_specs=vmem,
            scratch_shapes=[
                pltpu.VMEM((ROWS, D), bf),
                pltpu.VMEM((2, D, F), bf),
                pltpu.VMEM((2, ROWS, max(width for width, _ in HIDDEN)), jnp.float32),
                pltpu.VMEM((F, D), bf),
                pltpu.VMEM((ROWS, F), bf),
                chunks(jnp.float32),
                chunks(bf),
                chunks(bf),
                chunks(bf),
                chunks(bf),
                pltpu.VMEM((2, N * ROWS, C), bf),
                pltpu.VMEM((ROWS, C), bf),
                dma((1 + sum(len(depths) for _, depths in HIDDEN) + len(DOWN),)),
                dma((1 + max(len(groups) for groups in GROUPS),)),
                dma((len(DETOUR),)),
            ],
            compiler_params=pltpu.CompilerParams(
                collective_id=0, has_side_effects=True, vmem_limit_bytes=50 * 2**20
            ),
            name="block",
        )(hbm(x), hbm(w_gate), hbm(w_up), hbm(w_down))

    return jax.shard_map(
        step,
        mesh=mesh,
        in_specs=(P("dp", None), P(None, "tp"), P(None, "tp"), P("tp", None)),
        out_specs=P("dp", None),
        check_vma=False,
    )
```

```python
import jax
import jax.numpy as jnp
from jax import lax
from jax.experimental import pallas as pl
from jax.experimental.pallas import tpu as pltpu
from jax.sharding import PartitionSpec as P

ROWS = 128
D = 2048
F = 1536
HIDDEN = ((768, (1024, 1024)), (768, (768, 512, 256, 256, 256)))
DOWN = (256, 256, 512, 1024)
STEPS = ((0, 1), (2, 3), (4, 5, 6, 7), (8, 9, 10, 11), (12, 13, 14, 15))
LENT = 4
C = 128
N = D // C
SPLIT = (0, 1)
LAG = ((1, 1, 0, 1, 1), (2, 2, 2, 2, 2))

CUT = {4: 48}
GROUPS = (((0, 2, 6), (8, 10), (4, 20)), ((5, 7, 9, 11), (12, 13)))
DIRECT = (1, 3)
SHARED = (14, 15)
DETOUR = (4, 20)
RELAY_STEP = 3
SOURCE, RELAY, TARGET, GIVER = ({"dp": d, "tp": t} for d, t in ((0, 2), (1, 3), (0, 1), (0, 0)))
MESH = pl.DeviceIdType.MESH
scope = jax.named_scope
OWNER = {k: c for c in range(2) for group in GROUPS[c] for k in group} | {k: 1 for k in DIRECT + SHARED}


def rows(k):
    cut = CUT.get(k % N, ROWS)
    return (0, cut) if k < N else (cut, ROWS - cut)


def stored(k):
    first, n = rows(k)
    return pl.ds((k % N) * ROWS + first, n)


def in_y(k):
    return pl.ds(*rows(k)), pl.ds((k % N) * C, C)


def size(pieces):
    return sum(rows(k)[1] for k in pieces)


def pieces_of(chunks):
    return [k for k in list(chunks) + [N + k for k in chunks if k in CUT]]


def block(x_hbm, wg_hbm, wu_hbm, wd_hbm, out, xv, guv, part, wdv, h, own, tsend, trecv, ssend, srecv, drecv,
          relayed, in_sem, s_sem, relay_sem):
    me = lax.axis_index("tp")
    dp = lax.axis_index("dp")
    at_place = lambda place: jnp.logical_and(dp == place["dp"], me == place["tp"])
    not_at = lambda place: jnp.logical_or(dp != place["dp"], me != place["tp"])
    core = lax.rem(me, 2)
    sib = me + 1 - 2 * core
    opp = lax.rem(me + 2, 4)
    cross = 3 - me
    f32 = jnp.float32
    t_sem, send_sem, y_sem = in_sem, in_sem.at[LENT], in_sem.at[LENT + 1]

    barrier = pltpu.get_barrier_semaphore()

    def announce():
        for other in (sib, opp, cross):
            pl.semaphore_signal(barrier, inc=1, device_id={"tp": other}, device_id_type=MESH)
        for receiver, sender in ((RELAY, SOURCE), (TARGET, RELAY)):

            @pl.when(at_place(receiver))
            def _(sender=sender):
                pl.semaphore_signal(barrier, inc=1, device_id=sender, device_id_type=MESH)

    loads = []

    def load(ref, *pairs):
        loads.append((ref, pairs))
        return len(loads) - 1

    def start(i):
        for src, dst in loads[i][1]:
            pltpu.make_async_copy(src, dst, in_sem.at[i]).start()

    def loaded(i):
        ref = loads[i][0]
        pltpu.make_async_copy(ref, ref, in_sem.at[i]).wait()

    x_copy = load(xv, (x_hbm, xv))
    hidden, at = [], 0
    for width, depths in HIDDEN:
        cols, top, pieces = pl.ds(at, width), 0, []
        for depth in depths:
            deep = pl.ds(top, depth)
            n = load(
                guv.at[:, deep, cols],
                (wg_hbm.at[deep, cols], guv.at[0, deep, cols]),
                (wu_hbm.at[deep, cols], guv.at[1, deep, cols]),
            )
            pieces.append((n, top, depth))
            top += depth
        hidden.append((at, width, pieces))
        at += width
    down, at = {}, 0
    for width in DOWN:
        cols = pl.ds(at, width)
        down[at // C] = load(wdv.at[:, cols], (wd_hbm.at[:, cols], wdv.at[:, cols]))
        at += width
    for i in range(len(loads)):
        start(i)

    with scope("wait_x"):
        loaded(x_copy)
    for c, (at, width, pieces) in enumerate(hidden):
        cols = slice(at, at + width)
        for n, top, depth in pieces:
            with scope(f"wait_g{c}_{top}"):
                loaded(n)
            if n == LENT - 1:
                announce()
            with scope(f"hid{c}_{top}"):
                deep = slice(top, top + depth)
                gate = jnp.dot(xv[:, deep], guv[0, deep, cols], preferred_element_type=f32)
                up = jnp.dot(xv[:, deep], guv[1, deep, cols], preferred_element_type=f32)
                if top > 0:
                    gate, up = gate + part[0, :, :width], up + part[1, :, :width]
                if top + depth < D:
                    part[0, :, :width], part[1, :, :width] = gate, up
                else:
                    h[:, cols] = (jax.nn.silu(gate) * up).astype(jnp.bfloat16)
    def remote(src, dst, recv, to):
        return pltpu.make_async_remote_copy(
            src_ref=src,
            dst_ref=dst,
            send_sem=send_sem,
            recv_sem=recv,
            device_id=to if isinstance(to, dict) else {"tp": to},
            device_id_type=MESH,
        )

    def some(n):
        return tsend.at[pl.ds(0, n)], trecv.at[pl.ds(0, n)]

    def wait_recv(sem, n):
        remote(*some(n), sem, sib).wait_recv()

    group_of = {k: g for c in range(2) for g, group in enumerate(GROUPS[c]) for k in group}
    relay_sems = (s_sem.at[group_of[DETOUR[0]]], relay_sem)
    shared_sem = s_sem.at[max(len(groups) for groups in GROUPS)]
    t_slot = lambda j, c: t_sem.at[j - min(i for i in range(len(STEPS)) if summed(i, c))]
    s_copy = lambda k, to: remote(
        ssend.at[stored(k)], srecv.at[stored(k)], shared_sem if k in SHARED else s_sem.at[group_of[k]], to
    )
    d_sem = t_sem.at[len(STEPS) - 2]
    sent = {0: 0, 1: 0}

    def summed(j, c):
        return [k for k in pieces_of(STEPS[j]) if OWNER[k] == c and k not in DIRECT]

    def term(j):
        chunks = STEPS[j]
        if chunks[0] in down:
            with scope(f"wait_d{j}"):
                loaded(down[chunks[0]])
        with scope(f"down{j}"):
            cols = slice(chunks[0] * C, (chunks[-1] + 1) * C)
            if j in SPLIT:
                width = len(chunks) * C
                half = [slice(0, F // 2), slice(F // 2, F)]
                part[me // 4, :, :width] = jnp.dot(h[:, half[0]], wdv[half[0], cols], preferred_element_type=f32)
                value = jnp.dot(h[:, half[1]], wdv[half[1], cols], preferred_element_type=f32) + part[0, :, :width]
            else:
                value = jnp.dot(h[...], wdv[:, cols], preferred_element_type=f32)
            for i, k in enumerate(chunks):
                at = slice(k * ROWS, (k + 1) * ROWS)
                if k not in DIRECT:
                    own[at] = value[:, i * C : (i + 1) * C]
                tsend[at] = value[:, i * C : (i + 1) * C].astype(jnp.bfloat16)
            if j == 0:
                more = jnp.logical_or(at_place(SOURCE), at_place(RELAY)).astype(jnp.int32)
                pl.semaphore_wait(barrier, 3 + more)
            pieces = pieces_of(chunks)
            for c in range(2):

                @pl.when(core == c)
                def _(c=c):
                    for k in pieces:
                        if k in DIRECT:
                            place = drecv.at[c, stored(k)]
                            remote(tsend.at[stored(k)], place, d_sem, opp if c == OWNER[k] else cross).start()
                            sent[c] += size([k])
                    for k in pieces:
                        if OWNER[k] != c:
                            sem = d_sem if k in DIRECT else t_slot(j, OWNER[k])
                            remote(tsend.at[stored(k)], trecv.at[stored(k)], sem, sib).start()
                            sent[c] += size([k])

    def chip_sum(j, c):
        pieces = summed(j, c)
        if not pieces:
            return
        sent[c] += size(pieces) + 2 * size([k for k in pieces if k in SHARED])

        @pl.when(core == c)
        def _():
            if c == 1 and j == RELAY_STEP:

                @pl.when(at_place(RELAY))
                def _():
                    with scope("relay"):
                        for i, k in enumerate(DETOUR):
                            wait_recv(relay_sems[i], size([k]))
                            place = srecv.at[stored(k)]
                            remote(relayed.at[pl.ds(*rows(k))], place, s_sem.at[group_of[k]], TARGET).start()

            with scope(f"wait_t{j}"):
                wait_recv(t_slot(j, c), size(pieces))
            for k in pieces:
                with scope(f"sum{k}"):
                    at = stored(k)
                    ssend[at] = (own[at] + trecv[at].astype(f32)).astype(jnp.bfloat16)
                    if k in SHARED:
                        s_copy(k, cross).start()
                        remote(ssend.at[at], ssend.at[at], shared_sem, sib).start()
                    elif k in DETOUR:

                        @pl.when(at_place(SOURCE))
                        def _(k=k, at=at):
                            place = relayed.at[pl.ds(*rows(k))]
                            remote(ssend.at[at], place, relay_sems[DETOUR.index(k)], RELAY).start()

                        @pl.when(not_at(SOURCE))
                        def _(k=k):
                            s_copy(k, opp).start()

                        @pl.when(at_place(GIVER))
                        def _(at=at):
                            remote(ssend.at[at], ssend.at[at], relay_sems[0], sib).start()

                    else:
                        s_copy(k, opp).start()
            for k in pieces:
                if k in SHARED:
                    s_copy(k, opp).start()

    for j in range(len(STEPS) + 3):
        if j < len(STEPS):
            term(j)
        for c in range(2):
            for k in range(len(STEPS)):
                if k + LAG[c][k] == j:
                    chip_sum(k, c)

    for c in range(2):

        @pl.when(core == c)
        def _(c=c):
            def finish(k, here, there):
                with scope(f"fin{k}"):
                    out[in_y(k)] = (here + there).astype(jnp.bfloat16)
                    if k not in SHARED:
                        place = out.at[in_y(k)]
                        remote(place, place, y_sem, sib).start()
                        sent[c] += size([k])

            if c == 1 and DIRECT:
                with scope("wait_direct"):
                    wait_recv(d_sem, 3 * size(DIRECT))
                for k in DIRECT:
                    at = stored(k)
                    here = tsend[at].astype(f32) + trecv[at].astype(f32)
                    finish(k, here, drecv[1, at].astype(f32) + drecv[0, at].astype(f32))
            def finish_group(g, group):
                with scope(f"wait_s{group[0]}"):
                    wait_recv(s_sem.at[g], size(group))
                for k in group:
                    finish(k, ssend[stored(k)].astype(f32), srecv[stored(k)].astype(f32))

            for g, group in enumerate(GROUPS[c]):
                if DETOUR == group:
                    pl.when(not_at(GIVER))(lambda g=g, group=group: finish_group(g, group))
                else:
                    finish_group(g, group)
                if c == 1 and g == 0:

                    @pl.when(at_place(TARGET))
                    def _():
                        wait_recv(relay_sems[0], 2 * size(DETOUR))
                        for k in DETOUR:
                            finish(k, ssend[stored(k)].astype(f32), srecv[stored(k)].astype(f32))
                        sent[c] -= size(DETOUR)

            if SHARED:
                with scope("wait_shared"):
                    wait_recv(shared_sem, size(SHARED) * (2 - c))
            for k in SHARED:
                finish(k, ssend[stored(k)].astype(f32), srecv[stored(k)].astype(f32))
            with scope("drain"):
                come = size([k for k in OWNER if OWNER[k] != c and k not in SHARED])
                more = size(DETOUR)
                cases = [(at_place(GIVER), 0, more)] if c == 0 else [(at_place(TARGET), more, -more), (at_place(RELAY), more, 0)]
                cases.append((not_at(GIVER) if c == 0 else jnp.logical_and(not_at(TARGET), not_at(RELAY)), 0, 0))
                for place, extra_sent, extra_come in cases:

                    @pl.when(place)
                    def _(extra_sent=extra_sent, extra_come=extra_come):
                        total = sent[c] + extra_sent
                        while total:
                            n = min(total, N * ROWS)
                            remote(*some(n), y_sem, sib).wait_send()
                            total -= n
                        wait_recv(y_sem, come + extra_come)


def solution(mesh):
    bf = jnp.bfloat16
    dma = pltpu.SemaphoreType.DMA
    anywhere = pl.BlockSpec(memory_space=pl.ANY)
    vmem = pl.BlockSpec(memory_space=pltpu.VMEM)

    def step(x, w_gate, w_up, w_down):
        hbm = lambda a: pltpu.with_memory_space_constraint(a, pltpu.HBM)
        chunks = lambda dtype: pltpu.VMEM((N * ROWS, C), dtype)
        return pl.pallas_call(
            block,
            out_shape=pltpu.VMEM((ROWS, D), bf),
            in_specs=[anywhere] * 4,
            out_specs=vmem,
            scratch_shapes=[
                pltpu.VMEM((ROWS, D), bf),
                pltpu.VMEM((2, D, F), bf),
                pltpu.VMEM((2, ROWS, max(width for width, _ in HIDDEN)), jnp.float32),
                pltpu.VMEM((F, D), bf),
                pltpu.VMEM((ROWS, F), bf),
                chunks(jnp.float32),
                chunks(bf),
                chunks(bf),
                chunks(bf),
                chunks(bf),
                pltpu.VMEM((2, N * ROWS, C), bf),
                pltpu.VMEM((ROWS, C), bf),
                dma((1 + sum(len(depths) for _, depths in HIDDEN) + len(DOWN),)),
                dma((1 + max(len(groups) for groups in GROUPS),)),
                dma,
            ],
            compiler_params=pltpu.CompilerParams(
                collective_id=0, has_side_effects=True, vmem_limit_bytes=50 * 2**20
            ),
            name="block",
        )(hbm(x), hbm(w_gate), hbm(w_up), hbm(w_down))

    return jax.shard_map(
        step,
        mesh=mesh,
        in_specs=(P("dp", None), P(None, "tp"), P(None, "tp"), P("tp", None)),
        out_specs=P("dp", None),
        check_vma=False,
    )
```
